32 devices in a mesh: fsdp: 32 (over z, y, x, core).
Axes of the slice: x: 2, y: 2, z: 4, core: 2. Of those that a mesh axis runs over, the one named last changes fastest.
Arguments:
- tokens: int32 [32, 512], P('fsdp')
- positions: int32 [32, 512], P('fsdp')
- embed_table: bfloat16 [49152, 960], P('fsdp')
- attn_norm: bfloat16 [960], P('fsdp')
- w_query: bfloat16 [960, 960], P('fsdp')
- w_key: bfloat16 [960, 320], P('fsdp')
- w_value: bfloat16 [960, 320], P('fsdp')
- q_norm: bfloat16 [64], replicated
- k_norm: bfloat16 [64], replicated
- w_out: bfloat16 [960, 960], P('fsdp')
- mlp_norm: bfloat16 [960], P('fsdp')
- w_gate: bfloat16 [960, 2560], P('fsdp')
- w_up: bfloat16 [960, 2560], P('fsdp')
- w_down: bfloat16 [2560, 960], P('fsdp')
- dy_out: bfloat16 [32, 512, 960], P('fsdp')
Outputs:
- output 1: bfloat16 [32, 512, 960], P('fsdp')
- output 2: float32 [49152, 960], P('fsdp')
- output 3: float32 [960], P('fsdp')
- output 4: float32 [960, 960], P('fsdp')
- output 5: float32 [960, 320], P('fsdp')
- output 6: float32 [960, 320], P('fsdp')
- output 7: float32 [64], replicated
- output 8: float32 [64], replicated
- output 9: float32 [960, 960], P('fsdp')
- output 10: float32 [960], P('fsdp')
- output 11: float32 [960, 2560], P('fsdp')
- output 12: float32 [960, 2560], P('fsdp')
- output 13: float32 [2560, 960], P('fsdp')
All inputs are finite; a program needn't handle non-finite values.
Results may differ from the reference program's by a relative error of at most 0.0180273.
Values are sent between devices in bfloat16 or wider.
A program may use at most 1 GiB of HBM per device.

```python
import math
import jax
import jax.numpy as jnp
from jax import lax

D = 960
HEADS = 15
KV_HEADS = 5
HEAD = 64
FF = 2560
VOCAB = 49152
VOCAB_P = 49152
GROUP = 32
BATCH_DEV = 1
SEQ = 512

BATCH = GROUP * BATCH_DEV
Q_PER_KV = HEADS // KV_HEADS
ROWS_SHARD = VOCAB_P // GROUP
DOC_SPAN = max(SEQ // 4, 2)
NORM_EPS = 1e-6
ROPE_THETA = 1.0e6


def draw_tokens(rng_key):
    key_list = jax.random.split(rng_key, 4)
    id_top = jax.random.randint(key_list[0], (BATCH, SEQ), 1, VOCAB + 1)
    id_mid = jax.random.randint(key_list[1], (BATCH, SEQ), 0, id_top)
    token_ids = jax.random.randint(key_list[2], (BATCH, SEQ), 0, id_mid + 1)
    shard_lo = (jnp.arange(BATCH) % GROUP) * ROWS_SHARD
    shard_hi = jnp.minimum(shard_lo + ROWS_SHARD, VOCAB)
    cover_ids = jax.random.randint(key_list[3], (BATCH,), shard_lo, shard_hi)
    token_ids = token_ids.at[:, 0].set(cover_ids)
    return token_ids.at[BATCH - 1, SEQ - 1].set(VOCAB - 1).astype(jnp.int32)


def draw_positions(rng_key):
    seq_idx = jnp.arange(SEQ, dtype=jnp.int32)[None, :]
    starts = (jax.random.randint(rng_key, (BATCH, SEQ), 0, DOC_SPAN) == 0) | (seq_idx == 0)
    last_start = lax.cummax(jnp.where(starts, seq_idx, 0), axis=1)
    return (seq_idx - last_start).astype(jnp.int32)


def setup_inputs(seed: int = 0) -> dict:
    key_list = jax.random.split(jax.random.key(seed), 16)

    def weight(key_idx, arr_shape, fan_in):
        return (jax.random.normal(key_list[key_idx], arr_shape, jnp.float32) * fan_in ** -0.5).astype(jnp.bfloat16)

    def gain_vec(key_idx, vec_len):
        return (1.0 + 0.25 * jax.random.normal(key_list[key_idx], (vec_len,), jnp.float32)).astype(jnp.bfloat16)

    table_f = jax.random.normal(key_list[2], (VOCAB_P, D), jnp.float32)
    table_f = jnp.where(jnp.arange(VOCAB_P)[:, None] < VOCAB, table_f, 0.0)
    return {
        'tokens': draw_tokens(key_list[0]),
        'positions': draw_positions(key_list[1]),
        'embed_table': table_f.astype(jnp.bfloat16),
        'attn_norm': gain_vec(3, D),
        'w_query': weight(4, (D, HEADS * HEAD), D),
        'w_key': weight(5, (D, KV_HEADS * HEAD), D),
        'w_value': weight(6, (D, KV_HEADS * HEAD), D),
        'q_norm': gain_vec(7, HEAD),
        'k_norm': gain_vec(8, HEAD),
        'w_out': weight(9, (HEADS * HEAD, D), HEADS * HEAD),
        'mlp_norm': gain_vec(10, D),
        'w_gate': weight(11, (D, FF), D),
        'w_up': weight(12, (D, FF), D),
        'w_down': weight(13, (FF, D), FF),
        'dy_out': jax.random.normal(key_list[14], (BATCH, SEQ, D), jnp.float32).astype(jnp.bfloat16),
    }


def to_bf16(values):
    return values + lax.stop_gradient(values.astype(jnp.bfloat16).astype(jnp.float32) - values)


def rms_scale(values, norm_gain):
    inv_rms = lax.rsqrt(jnp.mean(values * values, axis=-1, keepdims=True) + NORM_EPS)
    return values * inv_rms * norm_gain


def rope_tables(positions):
    half_dim = HEAD // 2
    inv_freq = jnp.exp(jnp.arange(half_dim, dtype=jnp.float32) * (-2.0 * math.log(ROPE_THETA) / HEAD))
    angles = positions.astype(jnp.float32)[:, :, None] * inv_freq
    return jnp.cos(angles), jnp.sin(angles)


def rotate(values, cos_t, sin_t):
    half_dim = values.shape[-1] // 2
    lead_half = values[..., :half_dim]
    tail_half = values[..., half_dim:]
    return jnp.concatenate([lead_half * cos_t - tail_half * sin_t, tail_half * cos_t + lead_half * sin_t], axis=-1)


def seq_attend(operands):
    q_seq, k_seq, v_seq = operands
    scores = jnp.einsum('qgrh,kgh->grqk', q_seq, k_seq) * (HEAD ** -0.5)
    causal = jnp.arange(SEQ)[:, None] >= jnp.arange(SEQ)[None, :]
    scores = jnp.where(causal, scores, -1e30)
    attn_probs = to_bf16(jax.nn.softmax(scores, axis=-1))
    return to_bf16(jnp.einsum('grqk,kgh->qgrh', attn_probs, v_seq))


def reference(tokens, positions, embed_table, attn_norm, w_query, w_key, w_value, q_norm, k_norm, w_out, mlp_norm, w_gate, w_up, w_down, dy_out):
    cos_t, sin_t = rope_tables(positions)
    cos_q = cos_t[:, :, None, None, :]
    sin_q = sin_t[:, :, None, None, :]
    cos_k = cos_t[:, :, None, :]
    sin_k = sin_t[:, :, None, :]

    def layer_fwd(x_emb, g_attn, wt_query, wt_key, wt_value, g_query, g_key, wt_out, g_mlp, wt_gate, wt_up, wt_down):
        normed = to_bf16(rms_scale(x_emb, g_attn)).reshape(BATCH * SEQ, D)
        q_proj = to_bf16(jnp.dot(normed, wt_query, preferred_element_type=jnp.float32)).reshape(BATCH, SEQ, KV_HEADS, Q_PER_KV, HEAD)
        k_proj = to_bf16(jnp.dot(normed, wt_key, preferred_element_type=jnp.float32)).reshape(BATCH, SEQ, KV_HEADS, HEAD)
        v_proj = to_bf16(jnp.dot(normed, wt_value, preferred_element_type=jnp.float32)).reshape(BATCH, SEQ, KV_HEADS, HEAD)
        q_rot = to_bf16(rotate(rms_scale(q_proj, g_query), cos_q, sin_q))
        k_rot = to_bf16(rotate(rms_scale(k_proj, g_key), cos_k, sin_k))
        attn_heads = lax.map(jax.checkpoint(seq_attend), (q_rot, k_rot, v_proj))
        attn_proj = jnp.dot(attn_heads.reshape(BATCH * SEQ, HEADS * HEAD), wt_out, preferred_element_type=jnp.float32)
        hidden = to_bf16(x_emb + attn_proj.reshape(BATCH, SEQ, D))
        mlp_in = to_bf16(rms_scale(hidden, g_mlp)).reshape(BATCH * SEQ, D)
        gate_pre = jnp.dot(mlp_in, wt_gate, preferred_element_type=jnp.float32)
        up_proj = jnp.dot(mlp_in, wt_up, preferred_element_type=jnp.float32)
        mlp_act = to_bf16(jax.nn.silu(gate_pre) * up_proj)
        mlp_proj = jnp.dot(mlp_act, wt_down, preferred_element_type=jnp.float32)
        return to_bf16(hidden + mlp_proj.reshape(BATCH, SEQ, D))

    x_emb = jnp.take(embed_table, tokens, axis=0).astype(jnp.float32)
    params = [weight_arr.astype(jnp.float32) for weight_arr in (attn_norm, w_query, w_key, w_value, q_norm, k_norm, w_out, mlp_norm, w_gate, w_up, w_down)]
    layer_out, pullback = jax.vjp(layer_fwd, x_emb, *params)
    grad_list = pullback(dy_out.astype(jnp.float32))
    d_table = jax.ops.segment_sum(grad_list[0].reshape(BATCH * SEQ, D), tokens.reshape(BATCH * SEQ), num_segments=VOCAB_P)
    return (layer_out.astype(jnp.bfloat16), d_table, grad_list[1], grad_list[2], grad_list[3], grad_list[4], grad_list[5], grad_list[6], grad_list[7], grad_list[8], grad_list[9], grad_list[10], grad_list[11])
```

```python
import functools
import math
import jax
import jax.numpy as jnp
from jax import lax
from jax.experimental import pallas as pl
from jax.experimental.pallas import tpu as pltpu
from jax.sharding import PartitionSpec as P

NORM_EPS = 1e-6
ROPE_THETA = 1.0e6
AXIS_NAME = 'fsdp'
MESH = pl.DeviceIdType.MESH
NZ, NQ, NC = 4, 4, 2
N_DEV = NZ * NQ * NC
LANES = 128
SUBL = 8
VMEM_BYTES = 62 * 1024 * 1024
J_GATHER = (0, 1, 3, 2)
J_SCATTER = (2, 1, 3, 0)


def dev_id(z, q, c):
    y = lax.div(q, 2)
    x = lax.rem(q + y, 2)
    return z * 8 + y * 4 + x * 2 + c


def my_coords():
    me = lax.axis_index(AXIS_NAME)
    z = lax.div(me, 8)
    y = lax.rem(lax.div(me, 4), 2)
    x = lax.rem(lax.div(me, 2), 2)
    c = lax.rem(me, 2)
    q = y * 2 + lax.rem(x + y, 2)
    return me, z, q, c


def wrap4(value):
    return lax.rem(value + 16, 4)


def entry_barrier(z, q, c):
    barrier = pltpu.get_barrier_semaphore()
    peers = [dev_id(wrap4(z + k), q, c) for k in (1, 2, 3)]
    peers += [dev_id(z, wrap4(q + 1), c), dev_id(z, wrap4(q + 3), c), dev_id(z, q, 1 - c)]
    for peer in peers:
        pl.semaphore_signal(barrier, inc=1, device_id=(peer,), device_id_type=MESH)
    pl.semaphore_wait(barrier, len(peers))


def ids_kernel(src, dst, loc_sem, send_sem, recv_sem):
    me = lax.axis_index(AXIS_NAME)
    barrier = pltpu.get_barrier_semaphore()

    @pl.loop(1, N_DEV)
    def _(k):
        pl.semaphore_signal(barrier, inc=1, device_id=(lax.rem(me + k, N_DEV),), device_id_type=MESH)
    pl.semaphore_wait(barrier, N_DEV - 1)
    local = pltpu.make_async_copy(src, dst.at[me], loc_sem)
    local.start()

    @pl.loop(1, N_DEV)
    def _(k):
        pltpu.make_async_remote_copy(src_ref=src, dst_ref=dst.at[me], send_sem=send_sem.at[k], recv_sem=recv_sem.at[k],
                                     device_id=(lax.rem(me + k, N_DEV),), device_id_type=MESH).start()
    local.wait()

    @pl.loop(1, N_DEV)
    def _(k):
        copy = pltpu.make_async_remote_copy(src_ref=src, dst_ref=dst.at[lax.rem(me + N_DEV - k, N_DEV)], send_sem=send_sem.at[k],
                                            recv_sem=recv_sem.at[k], device_id=(lax.rem(me + k, N_DEV),), device_id_type=MESH)
        copy.wait_send()
        copy.wait_recv()


def gather_ids(block):
    return pl.pallas_call(
        ids_kernel,
        out_shape=jax.ShapeDtypeStruct((N_DEV,) + block.shape, block.dtype),
        in_specs=[pl.BlockSpec(memory_space=pltpu.VMEM)],
        out_specs=pl.BlockSpec(memory_space=pltpu.VMEM),
        scratch_shapes=[pltpu.SemaphoreType.DMA, pltpu.SemaphoreType.DMA((N_DEV,)), pltpu.SemaphoreType.DMA((N_DEV,))],
        compiler_params=pltpu.CompilerParams(collective_id=0, has_side_effects=True),
        name='gather_ids',
    )(block)


def weights_kernel(n_arr, *refs):
    ins = refs[:n_arr]
    outs = refs[n_arr:2 * n_arr]
    loc_sem, z_send, z_recv, r_send, r_recv, p_send, p_recv = refs[2 * n_arr:]
    me, z, q, c = my_coords()
    step_dir = 1 - 2 * c
    nxt = dev_id(z, wrap4(q + step_dir), c)
    mate = dev_id(z, q, 1 - c)
    entry_barrier(z, q, c)

    def remote(src, dst, send, recv, target):
        return pltpu.make_async_remote_copy(src_ref=src, dst_ref=dst, send_sem=send, recv_sem=recv, device_id=(target,), device_id_type=MESH)

    def block_at(j, s):
        return dev_id(wrap4(z - j), wrap4(q - step_dir * s), c)

    def source(a, j, s):
        return ins[a] if (j, s) == (0, 0) else outs[a].at[block_at(j, s)]

    def ring(a, j, s):
        return remote(source(a, j, s), outs[a].at[block_at(j, s)], r_send.at[a, s, j], r_recv.at[a, s, j], nxt)

    def ring_in(a, j, s):
        dst = outs[a].at[block_at(j, s + 1)]
        return remote(dst, dst, r_send.at[a, s, j], r_recv.at[a, s, j], nxt)

    def pair(a, j, s):
        return remote(source(a, j, s), outs[a].at[block_at(j, s)], p_send.at[a, s, j], p_recv.at[a, s, j], mate)

    def pair_in(a, j, s):
        dst = outs[a].at[dev_id(wrap4(z - j), wrap4(q + step_dir * s), 1 - c)]
        return remote(dst, dst, p_send.at[a, s, j], p_recv.at[a, s, j], mate)

    def column(a, k):
        return remote(ins[a], outs[a].at[me], z_send.at[a, k - 1], z_recv.at[a, k - 1], dev_id(wrap4(z + k), q, c))

    def column_in(a, k):
        dst = outs[a].at[dev_id(wrap4(z - k), q, c)]
        return remote(dst, dst, z_send.at[a, k - 1], z_recv.at[a, k - 1], dev_id(wrap4(z + k), q, c))

    arrays = range(n_arr)
    local = [pltpu.make_async_copy(ins[a], outs[a].at[me], loc_sem.at[a]) for a in arrays]
    for a in arrays:
        ring(a, 0, 0).start()
    for k in (1, 3, 2):
        for a in arrays:
            column(a, k).start()
    for a in arrays:
        local[a].start()
        pair(a, 0, 0).start()

    groups = [(0, 0)]
    for pos, j in enumerate(J_GATHER):
        groups += [(j, 1), (j, 2)]
        if pos + 1 < NZ:
            groups.append((J_GATHER[pos + 1], 0))
        groups.append((j, 3))
    for j, s in groups[1:]:
        for a in arrays:
            if s == 0:
                column_in(a, j).wait_recv()
            else:
                ring_in(a, j, s - 1).wait_recv()
            if s < 3:
                ring(a, j, s).start()
            pair(a, j, s).start()
    for a in arrays:
        local[a].wait()
        for j in range(NZ):
            for s in range(4):
                pair_in(a, j, s).wait_recv()
                pair(a, j, s).wait_send()
                if s < 3:
                    ring(a, j, s).wait_send()
        for k in (1, 2, 3):
            column(a, k).wait_send()


def gather_blocks(blocks, collective_id, name):
    n_arr = len(blocks)
    out_shape = tuple(jax.ShapeDtypeStruct((N_DEV,) + b.shape, b.dtype) for b in blocks)
    dma = pltpu.SemaphoreType.DMA
    return pl.pallas_call(
        functools.partial(weights_kernel, n_arr),
        out_shape=out_shape,
        in_specs=[pl.BlockSpec(memory_space=pltpu.VMEM)] * n_arr,
        out_specs=tuple(pl.BlockSpec(memory_space=pl.ANY) for _ in blocks),
        scratch_shapes=[dma((n_arr,)), dma((n_arr, 3)), dma((n_arr, 3)), dma((n_arr, 3, 4)), dma((n_arr, 3, 4)), dma((n_arr, 4, 4)), dma((n_arr, 4, 4))],
        compiler_params=pltpu.CompilerParams(collective_id=collective_id, has_side_effects=True, vmem_limit_bytes=8 * 1024 * 1024),
        name=name,
    )(*blocks)


def grads_kernel(n_arr, *refs):
    ins = refs[:n_arr]
    outs = refs[n_arr:2 * n_arr]
    scratch = refs[2 * n_arr:]
    own, mbuf, rbuf, zbuf = (scratch[i * n_arr:(i + 1) * n_arr] for i in range(4))
    o_sem, z_send, z_recv, r_send, r_recv, p_send, p_recv = scratch[4 * n_arr:]
    me, z, q, c = my_coords()
    step_dir = 1 - 2 * c
    nxt = dev_id(z, wrap4(q + step_dir), c)
    mate = dev_id(z, q, 1 - c)
    arrays = range(n_arr)
    groups = []
    for pos, j in enumerate(J_SCATTER):
        if pos == 0:
            groups.append((j, 0))
        groups += [(j, 1), (j, 2)]
        if pos + 1 < NZ:
            groups.append((J_SCATTER[pos + 1], 0))
        groups.append((j, 3))
    n_groups = len(groups)

    def remote(src, dst, send, recv, target):
        return pltpu.make_async_remote_copy(src_ref=src, dst_ref=dst, send_sem=send, recv_sem=recv, device_id=(target,), device_id_type=MESH)

    def own_load(g, a):
        j, s = groups[g]
        block = dev_id(wrap4(z + j), wrap4(q - step_dir * (1 + s)), c)
        return pltpu.make_async_copy(ins[a].at[block], own[a].at[g % 2], o_sem.at[a, g % 2])

    def pair(g, a):
        j, s = groups[g]
        block = dev_id(wrap4(z + j), wrap4(q + step_dir * (1 + s)), 1 - c)
        return remote(ins[a].at[block], mbuf[a].at[g], p_send.at[a, g], p_recv.at[a, g], mate)

    def place(j, s):
        return j * 3 + s

    def ring(g, a):
        j, s = groups[g]
        src = mbuf[a].at[g] if s == 0 else rbuf[a].at[place(j, s - 1)]
        return remote(src, rbuf[a].at[place(j, s)], r_send.at[a, place(j, s)], r_recv.at[a, place(j, s)], nxt)

    def column(a, j):
        return remote(rbuf[a].at[place(j, 2)], zbuf[a].at[j - 1], z_send.at[a, j - 1], z_recv.at[a, j - 1], dev_id(wrap4(z + j), q, c))

    def add_into(dst, others):
        rows = dst.shape[0]

        @pl.loop(0, rows // SUBL)
        def _(r):
            here = pl.ds(pl.multiple_of(r * SUBL, SUBL), SUBL)
            total = dst[here, :]
            for other in others:
                total = total + other[here, :]
            dst[here, :] = total

    for a in arrays:
        own_load(0, a).start()
    entry_barrier(z, q, c)
    for g in range(3):
        for a in arrays:
            pair(g, a).start()
    for g, (j, s) in enumerate(groups):
        for a in arrays:
            if g + 1 < n_groups:
                own_load(g + 1, a).start()
            if g + 3 < n_groups:
                pair(g + 3, a).start()
        for a in arrays:
            own_load(g, a).wait()
            pair(g, a).wait_recv()
            if s == 0:
                add_into(mbuf[a].at[g], [own[a].at[g % 2]])
            else:
                slot = place(j, s - 1)
                remote(rbuf[a].at[slot], rbuf[a].at[slot], r_send.at[a, slot], r_recv.at[a, slot], nxt).wait_recv()
                add_into(rbuf[a].at[slot], [own[a].at[g % 2], mbuf[a].at[g]])
            if s < 3:
                ring(g, a).start()
            elif j != 0:
                column(a, j).start()
    for a in arrays:
        for j in (1, 2, 3):
            column(a, j).wait_recv()
        rows = outs[a].shape[0]

        @pl.loop(0, rows // SUBL)
        def _(r):
            here = pl.ds(pl.multiple_of(r * SUBL, SUBL), SUBL)
            total = rbuf[a][place(0, 2), here, :]
            for k in range(3):
                total = total + zbuf[a][k, here, :]
            outs[a][here, :] = total
    for a in arrays:
        for g, (j, s) in enumerate(groups):
            pair(g, a).wait_send()
            if s < 3:
                ring(g, a).wait_send()
        for j in (1, 2, 3):
            column(a, j).wait_send()


def scatter_grads(parts):
    n_arr = len(parts)
    shapes = [p.shape[1:] for p in parts]
    dma = pltpu.SemaphoreType.DMA

    def bufs(count):
        return [pltpu.VMEM((count,) + s, jnp.float32) for s in shapes]

    return pl.pallas_call(
        functools.partial(grads_kernel, n_arr),
        out_shape=tuple(jax.ShapeDtypeStruct(s, jnp.float32) for s in shapes),
        in_specs=[pl.BlockSpec(memory_space=pl.ANY)] * n_arr,
        out_specs=tuple(pl.BlockSpec(memory_space=pltpu.VMEM) for _ in parts),
        scratch_shapes=bufs(2) + bufs(16) + bufs(12) + bufs(3) + [
            dma((n_arr, 2)), dma((n_arr, 3)), dma((n_arr, 3)), dma((n_arr, 12)), dma((n_arr, 12)), dma((n_arr, 16)), dma((n_arr, 16))],
        compiler_params=pltpu.CompilerParams(collective_id=2, has_side_effects=True, vmem_limit_bytes=VMEM_BYTES),
        name='scatter_grads',
    )(*parts)


X_CHUNKS = 4


def rows_kernel(ids, table, out, tab, first, rbuf, zbuf, loc_sem, t_send, t_recv, z_send, z_recv, r_send, r_recv):
    me, z, q, c = my_coords()
    step_dir = 1 - 2 * c
    nxt = dev_id(z, wrap4(q + step_dir), c)
    mate = dev_id(z, q, 1 - c)
    n_local = table.shape[0]
    seq = out.shape[0]
    step = seq // X_CHUNKS
    groups = []
    for pos, j in enumerate(J_SCATTER):
        if pos == 0:
            groups.append((j, 0))
        groups += [(j, 1), (j, 2)]
        if pos + 1 < NZ:
            groups.append((J_SCATTER[pos + 1], 0))
        groups.append((j, 3))

    def remote(src, dst, send, recv, target):
        return pltpu.make_async_remote_copy(src_ref=src, dst_ref=dst, send_sem=send, recv_sem=recv, device_id=(target,), device_id_type=MESH)

    mine = tab.at[pl.ds(c * n_local, n_local)]
    local = pltpu.make_async_copy(table, mine, loc_sem)
    local.start()
    entry_barrier(z, q, c)
    share = remote(table, mine, t_send, t_recv, mate)
    share.start()
    local.wait()
    theirs = tab.at[pl.ds((1 - c) * n_local, n_local)]
    remote(table, theirs, t_send, t_recv, mate).wait_recv()

    def place(j, s):
        return j * 3 + s

    def part(ref, h):
        return ref.at[pl.ds(h * step, step)]

    def ring(j, s, h):
        src = first.at[j] if s == 0 else rbuf.at[place(j, s - 1)]
        return remote(part(src, h), part(rbuf.at[place(j, s)], h), r_send.at[place(j, s), h], r_recv.at[place(j, s), h], nxt)

    def column(j, h):
        return remote(part(rbuf.at[place(j, 2)], h), part(zbuf.at[j - 1], h), z_send.at[j - 1, h], z_recv.at[j - 1, h], dev_id(wrap4(z + j), q, c))

    for j, s in groups:
        block = dev_id(wrap4(z + j), wrap4(q - step_dir * (1 + s)), c)
        for h in range(X_CHUNKS):
            if s > 0:
                slot = place(j, s - 1)
                landed = part(rbuf.at[slot], h)
                remote(landed, landed, r_send.at[slot, h], r_recv.at[slot, h], nxt).wait_recv()
                dst = rbuf.at[slot]
            else:
                dst = first.at[j]

            @pl.loop(0, step // SUBL)
            def _(t):
                for u in range(SUBL):
                    k = h * step + t * SUBL + u
                    row = ids[block * seq + k]
                    held = jnp.logical_and(row >= 0, row < 2 * n_local)
                    value = tab[jnp.clip(row, 0, 2 * n_local - 1)]
                    base = jnp.zeros_like(value) if s == 0 else dst[k]
                    dst[k] = jnp.where(held, value, base)
            if s < 3:
                ring(j, s, h).start()
            elif j != 0:
                column(j, h).start()
    for h in range(X_CHUNKS):
        for j in (1, 2, 3):
            column(j, h).wait_recv()

        @pl.loop(0, step // SUBL)
        def _(t):
            here = pl.ds(h * step + t * SUBL, SUBL)
            total = rbuf[place(0, 2), here]
            for k in range(3):
                total = total + zbuf[k, here]
            out[here] = total
    for h in range(X_CHUNKS):
        for j in range(NZ):
            for s in range(3):
                ring(j, s, h).wait_send()
        for j in (1, 2, 3):
            column(j, h).wait_send()
    share.wait_send()


def fetch_rows(ids, table, seq):
    row = table.shape[1:]
    dma = pltpu.SemaphoreType.DMA
    vmem = pl.BlockSpec(memory_space=pltpu.VMEM)
    return pl.pallas_call(
        rows_kernel,
        out_shape=jax.ShapeDtypeStruct((seq,) + row, table.dtype),
        in_specs=[pl.BlockSpec(memory_space=pltpu.SMEM), vmem],
        out_specs=vmem,
        scratch_shapes=[pltpu.VMEM((2 * table.shape[0],) + row, table.dtype), pltpu.VMEM((4, seq) + row, table.dtype), pltpu.VMEM((12, seq) + row, table.dtype),
                        pltpu.VMEM((3, seq) + row, table.dtype), dma, dma, dma, dma((3, X_CHUNKS)), dma((3, X_CHUNKS)), dma((12, X_CHUNKS)), dma((12, X_CHUNKS))],
        compiler_params=pltpu.CompilerParams(collective_id=3, has_side_effects=True, vmem_limit_bytes=48 * 1024 * 1024),
        name='fetch_rows',
    )(ids, table)


N_ACC = 4
DX_CHUNKS = 4


def add_kernel(keys, starts, counts, base_ref, *refs):
    rows = refs[:DX_CHUNKS]
    out = refs[DX_CHUNKS]
    accs = refs[DX_CHUNKS + 1:DX_CHUNKS + 1 + N_ACC]
    buf, sem = refs[DX_CHUNKS + 1 + N_ACC:]
    n_out, width = out.shape
    seq = buf.shape[1] // SUBL
    part = buf.shape[1] // DX_CHUNKS
    base = base_ref[0]

    def load(i, h):
        slot = lax.rem(i, 2)
        return pltpu.make_async_copy(rows[h].at[i], buf.at[slot, pl.ds(h * part, part)], sem.at[slot, h])

    for h in range(DX_CHUNKS):
        load(0, h).start()

    @pl.loop(0, n_out)
    def _(r):
        for acc in accs:
            acc[pl.ds(pl.multiple_of(r * SUBL, SUBL), SUBL), :] = jnp.zeros((SUBL, LANES), jnp.float32)

    def add_row(i, k, acc):
        key = keys[i * seq + k]
        row = pl.multiple_of((lax.shift_right_logical(key, 9) - base) * SUBL, SUBL)
        src = pl.multiple_of(jnp.bitwise_and(key, 511) * SUBL, SUBL)
        acc[pl.ds(row, SUBL), :] += buf[lax.rem(i, 2), pl.ds(src, SUBL), :]

    @pl.loop(0, N_DEV)
    def _(i):
        @pl.when(i + 1 < N_DEV)
        def _():
            for h in range(DX_CHUNKS):
                load(i + 1, h).start()
        for h in range(DX_CHUNKS):
            load(i, h).wait()
        start = starts[i]
        count = counts[i]
        full = lax.div(count, 8)

        @pl.loop(0, full)
        def _(t):
            for u in range(8):
                add_row(i, start + t * 8 + u, accs[u % N_ACC])

        @pl.loop(full * 8, count)
        def _(k):
            add_row(i, start + k, accs[0])

    @pl.loop(0, n_out // SUBL)
    def _(r):
        for j in range(SUBL):
            lanes = min(LANES, width - j * LANES)
            value = accs[0][pl.ds(r * (SUBL * SUBL) + j, SUBL, stride=SUBL), :]
            for acc in accs[1:]:
                value = value + acc[pl.ds(r * (SUBL * SUBL) + j, SUBL, stride=SUBL), :]
            out[pl.ds(pl.multiple_of(r * SUBL, SUBL), SUBL), pl.ds(j * LANES, lanes)] = value[:, :lanes]


def add_rows(keys, starts, counts, base, rows, n_out, width):
    smem = pl.BlockSpec(memory_space=pltpu.SMEM)
    seq_rows = DX_CHUNKS * rows[0].shape[1]
    return pl.pallas_call(
        add_kernel,
        out_shape=jax.ShapeDtypeStruct((n_out, width), jnp.float32),
        in_specs=[smem] * 4 + [pl.BlockSpec(memory_space=pl.ANY)] * DX_CHUNKS,
        out_specs=pl.BlockSpec(memory_space=pltpu.VMEM),
        scratch_shapes=[pltpu.VMEM((n_out * SUBL, LANES), jnp.float32)] * N_ACC + [
            pltpu.VMEM((2, seq_rows, LANES), jnp.float32), pltpu.SemaphoreType.DMA((2, DX_CHUNKS))],
        compiler_params=pltpu.CompilerParams(vmem_limit_bytes=VMEM_BYTES),
        name='add_rows',
    )(keys, starts, counts, base, *rows)


def rope_tables(positions, head_dim):
    half_dim = head_dim // 2
    inv_freq = jnp.exp(jnp.arange(half_dim, dtype=jnp.float32) * (-2.0 * math.log(ROPE_THETA) / head_dim))
    angles = positions.astype(jnp.float32)[:, None] * inv_freq
    return jnp.cos(angles), jnp.sin(angles)


def rotate(values, cos_t, sin_t):
    half_dim = values.shape[-1] // 2
    lead_half = values[..., :half_dim]
    tail_half = values[..., half_dim:]
    return jnp.concatenate([lead_half * cos_t - tail_half * sin_t, tail_half * cos_t + lead_half * sin_t], axis=-1)


def norm_fwd(values):
    values_f = values.astype(jnp.float32)
    inv_rms = lax.rsqrt(jnp.mean(values_f * values_f, axis=-1, keepdims=True) + NORM_EPS)
    return values_f * inv_rms, inv_rms


def norm_bwd(grad_out, normed, inv_rms, norm_gain):
    grad_normed = grad_out * norm_gain.astype(jnp.float32)
    mean_term = jnp.mean(grad_normed * normed, axis=-1, keepdims=True)
    return inv_rms * (grad_normed - normed * mean_term)


def attn_fwd(q_rot, k_rot, v_raw):
    seq_len = q_rot.shape[0]
    attn_scale = q_rot.shape[-1] ** -0.5
    scores = jnp.einsum('qgrh,kgh->grqk', q_rot, k_rot, preferred_element_type=jnp.float32) * attn_scale
    causal = lax.broadcasted_iota(jnp.int32, (seq_len, seq_len), 0) >= lax.broadcasted_iota(jnp.int32, (seq_len, seq_len), 1)
    attn_probs = jax.nn.softmax(jnp.where(causal, scores, -1e30), axis=-1)
    attn_heads = jnp.einsum('grqk,kgh->qgrh', attn_probs.astype(jnp.bfloat16), v_raw, preferred_element_type=jnp.float32)
    return attn_heads.astype(jnp.bfloat16), attn_probs


def attn_bwd(grad_b, q_rot, k_rot, v_raw, attn_probs):
    attn_scale = q_rot.shape[-1] ** -0.5
    probs_b = attn_probs.astype(jnp.bfloat16)
    grad_probs = jnp.einsum('qgrh,kgh->grqk', grad_b, v_raw, preferred_element_type=jnp.float32)
    grad_v = jnp.einsum('grqk,qgrh->kgh', probs_b, grad_b, preferred_element_type=jnp.float32)
    grad_scores = attn_probs * (grad_probs - jnp.sum(grad_probs * attn_probs, axis=-1, keepdims=True)) * attn_scale
    scores_b = grad_scores.astype(jnp.bfloat16)
    grad_q = jnp.einsum('grqk,kgh->qgrh', scores_b, k_rot, preferred_element_type=jnp.float32)
    grad_k = jnp.einsum('grqk,qgrh->kgh', scores_b, q_rot, preferred_element_type=jnp.float32)
    return grad_q, grad_k, grad_v


def dot_f32(lhs, rhs):
    return jnp.dot(lhs, rhs, preferred_element_type=jnp.float32)


def dot_t(lhs, rhs):
    return lax.dot_general(lhs, rhs, (((0,), (0,)), ((), ())), preferred_element_type=jnp.float32)


def dot_nt(lhs, rhs):
    return lax.dot_general(lhs, rhs, (((1,), (1,)), ((), ())), preferred_element_type=jnp.float32)


def pad_rows(shard, rows):
    return jnp.pad(shard, ((0, rows - shard.shape[0]), (0, 0)))


def solution(mesh):
    row_spec = P(AXIS_NAME, None)
    vec_spec = P(AXIS_NAME)
    full_spec = P(None)
    batch_spec = P(AXIS_NAME, None, None)
    weight_specs = (vec_spec, row_spec, row_spec, row_spec, full_spec, full_spec, row_spec, vec_spec, row_spec, row_spec, row_spec)

    def device_step(tokens, positions, table_shard, attn_norm_s, w_query, w_key, w_value, q_norm, k_norm, w_out, mlp_norm_s, w_gate, w_up, w_down, dy_out):
        me = lax.axis_index(AXIS_NAME)
        seq = tokens.shape[1]
        rows_local, dim = table_shard.shape
        part = dim // N_DEV
        part_p = -(-part // 16) * 16
        dim_p = part_p * N_DEV
        head_dim = q_norm.shape[0]
        n_q = w_query.shape[1]
        n_kv = w_key.shape[1]
        kv_heads = n_kv // head_dim
        q_per_kv = n_q // n_kv

        ids = tokens[0]
        order = jnp.arange(seq, dtype=jnp.int32)
        keys = ids * seq + order
        rank = jnp.sum((keys[None, :] < keys[:, None]).astype(jnp.int32), axis=1)
        sorted_keys = jnp.sum(jnp.where(rank[None, :] == order[:, None], keys[None, :], 0), axis=1)
        all_keys = gather_ids(jnp.concatenate([ids, sorted_keys]).reshape(2 * seq // LANES, LANES)).reshape(N_DEV, 2, seq)
        all_ids = all_keys[:, 0]
        all_keys = all_keys[:, 1]
        chip_ids = (all_ids - me // NC * (NC * rows_local)).reshape(-1)
        width_p = SUBL * LANES
        table_rows = jnp.pad(table_shard, ((0, 0), (0, width_p - dim))).reshape(rows_local, SUBL, LANES)
        x_emb = fetch_rows(chip_ids, table_rows, seq).reshape(seq, width_p)[:, :dim].astype(jnp.float32)
        low = me * (rows_local * seq)
        my_starts = jnp.sum((all_keys < low).astype(jnp.int32), axis=1)
        my_counts = jnp.sum((all_keys < low + rows_local * seq).astype(jnp.int32), axis=1) - my_starts

        norm_pad = ((0, 0), (0, LANES - part))
        gains = jnp.concatenate([jnp.pad(attn_norm_s[None], norm_pad), jnp.pad(mlp_norm_s[None], norm_pad), jnp.zeros((14, LANES), attn_norm_s.dtype)], axis=0)
        w_qkv = jnp.concatenate([w_query, w_key, w_value], axis=1)
        blocks = [gains, pad_rows(w_qkv, part_p), pad_rows(w_out, part_p), pad_rows(w_gate, part_p), pad_rows(w_up, part_p), w_down]
        gains_all, w_qkv_p, w_out_p, w_gate_p, w_up_p, w_down_f = gather_blocks(blocks, 1, 'gather_weights')
        attn_norm = gains_all[:, 0, :part].reshape(dim)
        mlp_norm = gains_all[:, 1, :part].reshape(dim)
        w_qkv_p, w_out_p, w_gate_p, w_up_p, w_down_f = (w.reshape(-1, w.shape[-1]) for w in (w_qkv_p, w_out_p, w_gate_p, w_up_p, w_down_f))

        wide_pos = jnp.arange(dim_p, dtype=jnp.int32)
        dim_pos = jnp.arange(dim, dtype=jnp.int32)
        spread = (wide_pos[None, :] == (dim_pos // part * part_p + dim_pos % part)[:, None]).astype(jnp.bfloat16)

        def widen(values):
            return dot_f32(values, spread).astype(jnp.bfloat16)

        def narrow(values):
            return values.reshape(seq, N_DEV, part_p)[:, :, :part].reshape(seq, dim)

        cos_t, sin_t = rope_tables(positions[0], head_dim)
        cos_q, sin_q = cos_t[:, None, None, :], sin_t[:, None, None, :]
        cos_k, sin_k = cos_t[:, None, :], sin_t[:, None, :]
        normed1, norm1_inv = norm_fwd(x_emb)
        attn_in = widen((normed1 * attn_norm.astype(jnp.float32)).astype(jnp.bfloat16))
        qkv = dot_f32(attn_in, w_qkv_p).astype(jnp.bfloat16)
        q_raw = qkv[:, :n_q].reshape(seq, kv_heads, q_per_kv, head_dim)
        k_raw = qkv[:, n_q:n_q + n_kv].reshape(seq, kv_heads, head_dim)
        v_raw = qkv[:, n_q + n_kv:].reshape(seq, kv_heads, head_dim)
        q_normed, q_inv = norm_fwd(q_raw)
        k_normed, k_inv = norm_fwd(k_raw)
        q_rot = rotate(q_normed * q_norm.astype(jnp.float32), cos_q, sin_q).astype(jnp.bfloat16)
        k_rot = rotate(k_normed * k_norm.astype(jnp.float32), cos_k, sin_k).astype(jnp.bfloat16)
        attn_heads, attn_probs = attn_fwd(q_rot, k_rot, v_raw)
        attn_flat = widen(attn_heads.reshape(seq, n_q))
        hidden = (x_emb + dot_f32(attn_flat, w_out_p)).astype(jnp.bfloat16)
        normed2, norm2_inv = norm_fwd(hidden)
        mlp_in = widen((normed2 * mlp_norm.astype(jnp.float32)).astype(jnp.bfloat16))
        gate_pre = dot_f32(mlp_in, w_gate_p)
        up_proj = dot_f32(mlp_in, w_up_p)
        mlp_act = (jax.nn.silu(gate_pre) * up_proj).astype(jnp.bfloat16)
        layer_out = (hidden.astype(jnp.float32) + dot_f32(mlp_act, w_down_f)).astype(jnp.bfloat16)

        dy = dy_out[0]
        grad_w_down = dot_t(mlp_act, dy)
        grad_act = dot_nt(dy, w_down_f)
        gate_sig = jax.nn.sigmoid(gate_pre)
        grad_gate = (grad_act * up_proj * gate_sig * (1.0 + gate_pre * (1.0 - gate_sig))).astype(jnp.bfloat16)
        grad_up = (grad_act * gate_pre * gate_sig).astype(jnp.bfloat16)
        grad_w_gate = dot_t(mlp_in, grad_gate)
        grad_w_up = dot_t(mlp_in, grad_up)
        grad_mlp_in = narrow(dot_nt(grad_gate, w_gate_p) + dot_nt(grad_up, w_up_p))
        grad_mlp_norm = jnp.sum(grad_mlp_in * normed2, axis=0)
        grad_hidden = dy.astype(jnp.float32) + norm_bwd(grad_mlp_in, normed2, norm2_inv, mlp_norm)
        hidden_b = grad_hidden.astype(jnp.bfloat16)
        grad_w_out = dot_t(attn_flat, hidden_b)
        grad_heads = dot_nt(dot_nt(hidden_b, w_out_p).astype(jnp.bfloat16), spread).astype(jnp.bfloat16).reshape(q_rot.shape)
        grad_q, grad_k, grad_v = attn_bwd(grad_heads, q_rot, k_rot, v_raw, attn_probs)
        grad_qt = rotate(grad_q, cos_q, -sin_q)
        grad_kt = rotate(grad_k, cos_k, -sin_k)
        grad_q_norm = jnp.sum(grad_qt * q_normed, axis=(0, 1, 2))
        grad_k_norm = jnp.sum(grad_kt * k_normed, axis=(0, 1))
        grad_q_raw = norm_bwd(grad_qt, q_normed, q_inv, q_norm).astype(jnp.bfloat16).reshape(seq, n_q)
        grad_k_raw = norm_bwd(grad_kt, k_normed, k_inv, k_norm).astype(jnp.bfloat16).reshape(seq, n_kv)
        grad_v_raw = grad_v.astype(jnp.bfloat16).reshape(seq, n_kv)
        grad_qkv = jnp.concatenate([grad_q_raw, grad_k_raw, grad_v_raw], axis=1)
        grad_attn_in = narrow(dot_nt(grad_qkv, w_qkv_p))
        grad_x_emb = grad_hidden + norm_bwd(grad_attn_in, normed1, norm1_inv, attn_norm)
        dx_rows = jnp.pad(grad_x_emb, ((0, 0), (0, width_p - dim))).reshape(DX_CHUNKS, seq * SUBL // DX_CHUNKS, LANES)
        dx_all = gather_blocks([dx_rows[h] for h in range(DX_CHUNKS)], 4, 'gather_dx')

        grad_attn_norm = jnp.sum(grad_attn_in * normed1, axis=0)
        grad_w_qkv = dot_t(attn_in, grad_qkv)
        small = jnp.stack([jnp.pad(grad_attn_norm.reshape(N_DEV, part), norm_pad), jnp.pad(grad_mlp_norm.reshape(N_DEV, part), norm_pad),
                           jnp.broadcast_to(jnp.concatenate([grad_q_norm, grad_k_norm])[None], (N_DEV, 2 * head_dim))], axis=1)
        small = jnp.pad(small, ((0, 0), (0, SUBL - 3), (0, 0)))
        parts = [small] + [g.reshape(N_DEV, -1, g.shape[-1]) for g in (grad_w_qkv, grad_w_out, grad_w_gate, grad_w_up, grad_w_down)]
        small_s, qkv_s, out_s, gate_s, up_s, down_s = scatter_grads(parts)
        d_table = add_rows(all_keys.reshape(-1), my_starts, my_counts, (me * rows_local).reshape(1), dx_all, rows_local, dim)
        return (layer_out[None], d_table, small_s[0, :part], qkv_s[:part, :n_q], qkv_s[:part, n_q:n_q + n_kv], qkv_s[:part, n_q + n_kv:],
                small_s[2, :head_dim], small_s[2, head_dim:], out_s[:part], small_s[1, :part], gate_s[:part], up_s[:part], down_s)

    return jax.shard_map(device_step, mesh=mesh, in_specs=(row_spec, row_spec, row_spec) + weight_specs + (batch_spec,), out_specs=(batch_spec, row_spec) + weight_specs, check_vma=False)
```

```python
import functools
import math
import jax
import jax.numpy as jnp
from jax import lax
from jax.experimental import pallas as pl
from jax.experimental.pallas import tpu as pltpu
from jax.sharding import PartitionSpec as P

NORM_EPS = 1e-6
ROPE_THETA = 1.0e6
AXIS_NAME = 'fsdp'
MESH = pl.DeviceIdType.MESH
NZ, NQ, NC = 4, 4, 2
N_DEV = NZ * NQ * NC
LANES = 128
SUBL = 8
VMEM_BYTES = 62 * 1024 * 1024
J_GATHER = (0, 1, 3, 2)
J_SCATTER = (2, 1, 3, 0)


def dev_id(z, q, c):
    y = lax.div(q, 2)
    x = lax.rem(q + y, 2)
    return z * 8 + y * 4 + x * 2 + c


def my_coords():
    me = lax.axis_index(AXIS_NAME)
    z = lax.div(me, 8)
    y = lax.rem(lax.div(me, 4), 2)
    x = lax.rem(lax.div(me, 2), 2)
    c = lax.rem(me, 2)
    q = y * 2 + lax.rem(x + y, 2)
    return me, z, q, c


def wrap4(value):
    return lax.rem(value + 16, 4)


def entry_barrier(z, q, c):
    barrier = pltpu.get_barrier_semaphore()
    peers = [dev_id(wrap4(z + k), q, c) for k in (1, 2, 3)]
    peers += [dev_id(z, wrap4(q + 1), c), dev_id(z, wrap4(q + 3), c), dev_id(z, q, 1 - c)]
    for peer in peers:
        pl.semaphore_signal(barrier, inc=1, device_id=(peer,), device_id_type=MESH)
    pl.semaphore_wait(barrier, len(peers))


def ids_kernel(src, dst, loc_sem, send_sem, recv_sem):
    me = lax.axis_index(AXIS_NAME)
    barrier = pltpu.get_barrier_semaphore()

    @pl.loop(1, N_DEV)
    def _(k):
        pl.semaphore_signal(barrier, inc=1, device_id=(lax.rem(me + k, N_DEV),), device_id_type=MESH)
    pl.semaphore_wait(barrier, N_DEV - 1)
    local = pltpu.make_async_copy(src, dst.at[me], loc_sem)
    local.start()

    @pl.loop(1, N_DEV)
    def _(k):
        pltpu.make_async_remote_copy(src_ref=src, dst_ref=dst.at[me], send_sem=send_sem.at[k], recv_sem=recv_sem.at[k],
                                     device_id=(lax.rem(me + k, N_DEV),), device_id_type=MESH).start()
    local.wait()

    @pl.loop(1, N_DEV)
    def _(k):
        copy = pltpu.make_async_remote_copy(src_ref=src, dst_ref=dst.at[lax.rem(me + N_DEV - k, N_DEV)], send_sem=send_sem.at[k],
                                            recv_sem=recv_sem.at[k], device_id=(lax.rem(me + k, N_DEV),), device_id_type=MESH)
        copy.wait_send()
        copy.wait_recv()


def gather_ids(block):
    return pl.pallas_call(
        ids_kernel,
        out_shape=jax.ShapeDtypeStruct((N_DEV,) + block.shape, block.dtype),
        in_specs=[pl.BlockSpec(memory_space=pltpu.VMEM)],
        out_specs=pl.BlockSpec(memory_space=pltpu.VMEM),
        scratch_shapes=[pltpu.SemaphoreType.DMA, pltpu.SemaphoreType.DMA((N_DEV,)), pltpu.SemaphoreType.DMA((N_DEV,))],
        compiler_params=pltpu.CompilerParams(collective_id=0, has_side_effects=True),
        name='gather_ids',
    )(block)


def blocks_kernel(n_a, n_b, stacked, *refs):
    n_arr = n_a + n_b
    if stacked:
        ins = [refs[0].at[a] for a in range(n_arr)]
        refs = refs[1:]
    else:
        ins = refs[:n_arr]
        refs = refs[n_arr:]
    outs = refs[:n_arr]
    loc_sem, az_send, az_recv, ar_send, ar_recv, ap_send, ap_recv, bz_send, bz_recv, br_send, br_recv, bp_send, bp_recv = refs[n_arr:]
    me, z, q, c = my_coords()
    step_dir = 1 - 2 * c
    nxt = dev_id(z, wrap4(q + step_dir), c)
    mate = dev_id(z, q, 1 - c)
    high = lax.div(z, 2)
    inner = lax.div(wrap4(z + 1), 2)
    entry_barrier(z, q, c)

    def remote(src, dst, send, recv, target):
        return pltpu.make_async_remote_copy(src_ref=src, dst_ref=dst, send_sem=send, recv_sem=recv, device_id=(target,), device_id_type=MESH)

    def source_z(t):
        if t == 0:
            return z
        base = t - inner if t == 1 else t
        return base + high * (3 - 2 * base)

    def block_at(t, s):
        return dev_id(source_z(t), wrap4(q - step_dir * s), c)

    def spot(a, t, s):
        return outs[a].at[block_at(t, s)]

    def source(a, t, s):
        return ins[a] if (t, s) == (0, 0) else spot(a, t, s)

    def ring(a, t, s):
        if a < n_a:
            sems = ar_send.at[a, s, t], ar_recv.at[a, s, t]
        else:
            sems = br_send.at[a - n_a, s], br_recv.at[a - n_a, s]
        return remote(source(a, t, s), spot(a, t, s), *sems, nxt)

    def ring_in(a, t, s):
        if a < n_a:
            sems = ar_send.at[a, s, t], ar_recv.at[a, s, t]
        else:
            sems = br_send.at[a - n_a, s], br_recv.at[a - n_a, s]
        return remote(spot(a, t, s + 1), spot(a, t, s + 1), *sems, nxt)

    def pair_sems(a, t, s):
        if a < n_a:
            return ap_send.at[a, s, t], ap_recv.at[a, s, t]
        return bp_send.at[a - n_a, s, t], bp_recv.at[a - n_a, s, t]

    def pair(a, t, s):
        return remote(source(a, t, s), spot(a, t, s), *pair_sems(a, t, s), mate)

    def pair_in(a, t, s):
        dst = outs[a].at[dev_id(source_z(t), wrap4(q + step_dir * s), 1 - c)]
        return remote(dst, dst, *pair_sems(a, t, s), mate)

    def column(a, t, s, up):
        side = 0 if up else 1
        if a < n_a:
            sems = az_send.at[a, side, t], az_recv.at[a, source_z(t)]
        else:
            sems = bz_send.at[a - n_a, s, side, t], bz_recv.at[a - n_a, s, source_z(t)]
        return remote(source(a, t, s), spot(a, t, s), *sems, dev_id(z + 1 if up else z - 1, q, c))

    def column_in(a, t, s):
        if a < n_a:
            sems = az_send.at[a, 0, t], az_recv.at[a, source_z(t)]
        else:
            sems = bz_send.at[a - n_a, s, 0, t], bz_recv.at[a - n_a, s, source_z(t)]
        return remote(spot(a, t, s), spot(a, t, s), *sems, mate)

    def spread(a, t, s, act):
        if t == 0:
            ups, downs = z < NZ - 1, z > 0
        else:
            ups = jnp.logical_and(inner == 1, source_z(t) < z)
            downs = jnp.logical_and(inner == 1, source_z(t) > z)

        @pl.when(ups)
        def _():
            act(column(a, t, s, True))

        @pl.when(downs)
        def _():
            act(column(a, t, s, False))

    def launch(copy):
        copy.start()

    def settle(copy):
        copy.wait_send()

    first = range(n_a)
    second = range(n_a, n_arr)
    local = [pltpu.make_async_copy(ins[a], outs[a].at[me], loc_sem.at[a]) for a in range(n_arr)]
    for a in list(second) + list(first):
        ring(a, 0, 0).start()
    for a in range(n_arr):
        spread(a, 0, 0, launch)
    for a in range(n_arr):
        local[a].start()
        pair(a, 0, 0).start()

    def ring_step(a, t, s):
        ring_in(a, t, s - 1).wait_recv()
        if s < 3:
            ring(a, t, s).start()
        pair(a, t, s).start()

    groups = []
    for t in range(NZ):
        groups += [(t, 1), (t, 2)]
        if t + 1 < NZ:
            groups.append((t + 1, 0))
        groups.append((t, 3))
    later = [(t, s) for t in (1, 2, 3) for s in range(4)]
    for t, s in groups:
        for a in first:
            if s == 0:
                column_in(a, t, 0).wait_recv()
                ring(a, t, 0).start()
                spread(a, t, 0, launch)
                pair(a, t, 0).start()
            else:
                ring_step(a, t, s)
        for a in second:
            if t == 0 and s > 0:
                ring_step(a, 0, s)
                spread(a, 0, s, launch)
            if (t, s) in ((0, 1), (0, 2)) or not later:
                continue
            tb, sb = later[0]
            if tb == 1 and sb == 3 and (t, s) == (1, 0):
                continue
            column_in(a, tb, sb).wait_recv()
            spread(a, tb, sb, launch)
            pair(a, tb, sb).start()
        if (t, s) not in ((0, 1), (0, 2)) and later:
            later.pop(0)
    for tb, sb in later:
        for a in second:
            column_in(a, tb, sb).wait_recv()
            spread(a, tb, sb, launch)
            pair(a, tb, sb).start()
    for a in range(n_arr):
        local[a].wait()
        for t in range(NZ):
            for s in range(4):
                pair_in(a, t, s).wait_recv()
                pair(a, t, s).wait_send()
                if s < 3 and (a < n_a or t == 0):
                    ring(a, t, s).wait_send()
                if s == 0 or a >= n_a:
                    spread(a, t, s, settle)


def gather_blocks(blocks, n_b, collective_id, name):
    stacked = not isinstance(blocks, list)
    n_arr = blocks.shape[0] if stacked else len(blocks)
    n_a = n_arr - n_b
    n_b1 = max(n_b, 1)
    out_shape = tuple(jax.ShapeDtypeStruct((N_DEV,) + blocks[a].shape, blocks[a].dtype) for a in range(n_arr))
    dma = pltpu.SemaphoreType.DMA
    operands = [blocks] if stacked else blocks
    return pl.pallas_call(
        functools.partial(blocks_kernel, n_a, n_b, stacked),
        out_shape=out_shape,
        in_specs=[pl.BlockSpec(memory_space=pltpu.VMEM)] * len(operands),
        out_specs=tuple(pl.BlockSpec(memory_space=pltpu.HBM) for _ in range(n_arr)),
        scratch_shapes=[dma((n_arr,)), dma((n_a, 2, 4)), dma((n_a, 4)), dma((n_a, 3, 4)), dma((n_a, 3, 4)), dma((n_a, 4, 4)), dma((n_a, 4, 4)),
                        dma((n_b1, 4, 2, 4)), dma((n_b1, 4, 4)), dma((n_b1, 3)), dma((n_b1, 3)), dma((n_b1, 4, 4)), dma((n_b1, 4, 4))],
        compiler_params=pltpu.CompilerParams(collective_id=collective_id, has_side_effects=True, vmem_limit_bytes=8 * 1024 * 1024),
        name=name,
    )(*operands)


def grads_kernel(n_arr, *refs):
    ins = refs[:n_arr]
    outs = refs[n_arr:2 * n_arr]
    scratch = refs[2 * n_arr:]
    own, mbuf, rbuf, zbuf = (scratch[i * n_arr:(i + 1) * n_arr] for i in range(4))
    o_sem, z_send, z_recv, r_send, r_recv, p_send, p_recv = scratch[4 * n_arr:]
    me, z, q, c = my_coords()
    step_dir = 1 - 2 * c
    nxt = dev_id(z, wrap4(q + step_dir), c)
    mate = dev_id(z, q, 1 - c)
    arrays = range(n_arr)
    groups = []
    for pos, j in enumerate(J_SCATTER):
        if pos == 0:
            groups.append((j, 0))
        groups += [(j, 1), (j, 2)]
        if pos + 1 < NZ:
            groups.append((J_SCATTER[pos + 1], 0))
        groups.append((j, 3))
    n_groups = len(groups)

    def remote(src, dst, send, recv, target):
        return pltpu.make_async_remote_copy(src_ref=src, dst_ref=dst, send_sem=send, recv_sem=recv, device_id=(target,), device_id_type=MESH)

    def own_load(g, a):
        j, s = groups[g]
        block = dev_id(wrap4(z + j), wrap4(q - step_dir * (1 + s)), c)
        return pltpu.make_async_copy(ins[a].at[block], own[a].at[g % 2], o_sem.at[a, g % 2])

    def pair(g, a):
        j, s = groups[g]
        block = dev_id(wrap4(z + j), wrap4(q + step_dir * (1 + s)), 1 - c)
        return remote(ins[a].at[block], mbuf[a].at[g], p_send.at[a, g], p_recv.at[a, g], mate)

    def place(j, s):
        return j * 3 + s

    def ring(g, a):
        j, s = groups[g]
        src = mbuf[a].at[g] if s == 0 else rbuf[a].at[place(j, s - 1)]
        return remote(src, rbuf[a].at[place(j, s)], r_send.at[a, place(j, s)], r_recv.at[a, place(j, s)], nxt)

    def column(a, j):
        return remote(rbuf[a].at[place(j, 2)], zbuf[a].at[j - 1], z_send.at[a, j - 1], z_recv.at[a, j - 1], dev_id(wrap4(z + j), q, c))

    def add_into(dst, others):
        rows = dst.shape[0]

        @pl.loop(0, rows // SUBL)
        def _(r):
            here = pl.ds(pl.multiple_of(r * SUBL, SUBL), SUBL)
            total = dst[here, :]
            for other in others:
                total = total + other[here, :]
            dst[here, :] = total

    for a in arrays:
        own_load(0, a).start()
    entry_barrier(z, q, c)
    for g in range(3):
        for a in arrays:
            pair(g, a).start()
    for g, (j, s) in enumerate(groups):
        for a in arrays:
            if g + 1 < n_groups:
                own_load(g + 1, a).start()
            if g + 3 < n_groups:
                pair(g + 3, a).start()
        for a in arrays:
            own_load(g, a).wait()
            pair(g, a).wait_recv()
            if s == 0:
                add_into(mbuf[a].at[g], [own[a].at[g % 2]])
            else:
                slot = place(j, s - 1)
                remote(rbuf[a].at[slot], rbuf[a].at[slot], r_send.at[a, slot], r_recv.at[a, slot], nxt).wait_recv()
                add_into(rbuf[a].at[slot], [own[a].at[g % 2], mbuf[a].at[g]])
            if s < 3:
                ring(g, a).start()
            elif j != 0:
                column(a, j).start()
    for a in arrays:
        for j in (1, 2, 3):
            column(a, j).wait_recv()
        rows = outs[a].shape[0]

        @pl.loop(0, rows // SUBL)
        def _(r):
            here = pl.ds(pl.multiple_of(r * SUBL, SUBL), SUBL)
            total = rbuf[a][place(0, 2), here, :]
            for k in range(3):
                total = total + zbuf[a][k, here, :]
            outs[a][here, :] = total
    for a in arrays:
        for g, (j, s) in enumerate(groups):
            pair(g, a).wait_send()
            if s < 3:
                ring(g, a).wait_send()
        for j in (1, 2, 3):
            column(a, j).wait_send()


def scatter_grads(parts):
    n_arr = len(parts)
    shapes = [p.shape[1:] for p in parts]
    dma = pltpu.SemaphoreType.DMA

    def bufs(count):
        return [pltpu.VMEM((count,) + s, jnp.float32) for s in shapes]

    return pl.pallas_call(
        functools.partial(grads_kernel, n_arr),
        out_shape=tuple(jax.ShapeDtypeStruct(s, jnp.float32) for s in shapes),
        in_specs=[pl.BlockSpec(memory_space=pltpu.HBM)] * n_arr,
        out_specs=tuple(pl.BlockSpec(memory_space=pltpu.VMEM) for _ in parts),
        scratch_shapes=bufs(2) + bufs(16) + bufs(12) + bufs(3) + [
            dma((n_arr, 2)), dma((n_arr, 3)), dma((n_arr, 3)), dma((n_arr, 12)), dma((n_arr, 12)), dma((n_arr, 16)), dma((n_arr, 16))],
        compiler_params=pltpu.CompilerParams(collective_id=2, has_side_effects=True, vmem_limit_bytes=VMEM_BYTES),
        name='scatter_grads',
    )(*parts)


X_CHUNKS = 4


def rows_kernel(ids, table, out, tab, first, rbuf, zbuf, loc_sem, t_send, t_recv, z_send, z_recv, r_send, r_recv):
    me, z, q, c = my_coords()
    step_dir = 1 - 2 * c
    nxt = dev_id(z, wrap4(q + step_dir), c)
    mate = dev_id(z, q, 1 - c)
    n_local = table.shape[0]
    seq = out.shape[0]
    step = seq // X_CHUNKS
    groups = []
    for pos, j in enumerate(J_SCATTER):
        if pos == 0:
            groups.append((j, 0))
        groups += [(j, 1), (j, 2)]
        if pos + 1 < NZ:
            groups.append((J_SCATTER[pos + 1], 0))
        groups.append((j, 3))

    def remote(src, dst, send, recv, target):
        return pltpu.make_async_remote_copy(src_ref=src, dst_ref=dst, send_sem=send, recv_sem=recv, device_id=(target,), device_id_type=MESH)

    mine = tab.at[pl.ds(c * n_local, n_local)]
    local = pltpu.make_async_copy(table, mine, loc_sem)
    local.start()
    entry_barrier(z, q, c)
    share = remote(table, mine, t_send, t_recv, mate)
    share.start()
    local.wait()
    theirs = tab.at[pl.ds((1 - c) * n_local, n_local)]
    remote(table, theirs, t_send, t_recv, mate).wait_recv()

    def place(j, s):
        return j * 3 + s

    def part(ref, h):
        return ref.at[pl.ds(h * step, step)]

    def ring(j, s, h):
        src = first.at[j] if s == 0 else rbuf.at[place(j, s - 1)]
        return remote(part(src, h), part(rbuf.at[place(j, s)], h), r_send.at[place(j, s), h], r_recv.at[place(j, s), h], nxt)

    def column(j, h):
        return remote(part(rbuf.at[place(j, 2)], h), part(zbuf.at[j - 1], h), z_send.at[j - 1, h], z_recv.at[j - 1, h], dev_id(wrap4(z + j), q, c))

    for j, s in groups:
        block = dev_id(wrap4(z + j), wrap4(q - step_dir * (1 + s)), c)
        for h in range(X_CHUNKS):
            if s > 0:
                slot = place(j, s - 1)
                landed = part(rbuf.at[slot], h)
                remote(landed, landed, r_send.at[slot, h], r_recv.at[slot, h], nxt).wait_recv()
                dst = rbuf.at[slot]
            else:
                dst = first.at[j]

            @pl.loop(0, step // SUBL)
            def _(t):
                for u in range(SUBL):
                    k = h * step + t * SUBL + u
                    row = ids[block * seq + k]
                    held = jnp.logical_and(row >= 0, row < 2 * n_local)
                    value = tab[jnp.clip(row, 0, 2 * n_local - 1)]
                    base = jnp.zeros_like(value) if s == 0 else dst[k]
                    dst[k] = jnp.where(held, value, base)
            if s < 3:
                ring(j, s, h).start()
            elif j != 0:
                column(j, h).start()
    for h in range(X_CHUNKS):
        for j in (1, 2, 3):
            column(j, h).wait_recv()

        @pl.loop(0, step // SUBL)
        def _(t):
            here = pl.ds(h * step + t * SUBL, SUBL)
            total = rbuf[place(0, 2), here]
            for k in range(3):
                total = total + zbuf[k, here]
            out[here] = total
    for h in range(X_CHUNKS):
        for j in range(NZ):
            for s in range(3):
                ring(j, s, h).wait_send()
        for j in (1, 2, 3):
            column(j, h).wait_send()
    share.wait_send()


def fetch_rows(ids, table, seq):
    row = table.shape[1:]
    dma = pltpu.SemaphoreType.DMA
    vmem = pl.BlockSpec(memory_space=pltpu.VMEM)
    return pl.pallas_call(
        rows_kernel,
        out_shape=jax.ShapeDtypeStruct((seq,) + row, table.dtype),
        in_specs=[pl.BlockSpec(memory_space=pltpu.SMEM), vmem],
        out_specs=vmem,
        scratch_shapes=[pltpu.VMEM((2 * table.shape[0],) + row, table.dtype), pltpu.VMEM((4, seq) + row, table.dtype), pltpu.VMEM((12, seq) + row, table.dtype),
                        pltpu.VMEM((3, seq) + row, table.dtype), dma, dma, dma, dma((3, X_CHUNKS)), dma((3, X_CHUNKS)), dma((12, X_CHUNKS)), dma((12, X_CHUNKS))],
        compiler_params=pltpu.CompilerParams(collective_id=3, has_side_effects=True, vmem_limit_bytes=48 * 1024 * 1024),
        name='fetch_rows',
    )(ids, table)


N_ACC = 4
DX_CHUNKS = 4


def pack_kernel(rank, dx, out, tmp):
    seq, width = dx.shape
    part = seq // DX_CHUNKS

    @pl.loop(0, seq // SUBL)
    def _(r):
        here = pl.ds(pl.multiple_of(r * SUBL, SUBL), SUBL)
        for j in range(SUBL):
            lanes = min(LANES, width - j * LANES)
            value = dx[here, pl.ds(j * LANES, lanes)]
            if lanes < LANES:
                value = jnp.concatenate([value, jnp.zeros((SUBL, LANES - lanes), value.dtype)], axis=1)
            tmp[pl.ds(r * (SUBL * SUBL) + j, SUBL, stride=SUBL), :] = value

    @pl.loop(0, seq // SUBL)
    def _(r):
        for u in range(SUBL):
            i = r * SUBL + u
            place = rank[i]
            row = pl.multiple_of(lax.rem(place, part) * SUBL, SUBL)
            out[lax.div(place, part), pl.ds(row, SUBL), :] = tmp[pl.ds(pl.multiple_of(i * SUBL, SUBL), SUBL), :]


def pack_rows(rank, dx):
    seq = dx.shape[0]
    vmem = pl.BlockSpec(memory_space=pltpu.VMEM)
    return pl.pallas_call(
        pack_kernel,
        out_shape=jax.ShapeDtypeStruct((DX_CHUNKS, seq * SUBL // DX_CHUNKS, LANES), dx.dtype),
        in_specs=[pl.BlockSpec(memory_space=pltpu.SMEM), vmem],
        out_specs=vmem,
        scratch_shapes=[pltpu.VMEM((seq * SUBL, LANES), dx.dtype)],
        compiler_params=pltpu.CompilerParams(vmem_limit_bytes=16 * 1024 * 1024),
        name='pack_rows',
    )(rank, dx)


OUT_ROWS = 128


def add_kernel(ids, starts, counts, *refs):
    rows = refs[:DX_CHUNKS]
    out = refs[DX_CHUNKS]
    accs = refs[DX_CHUNKS + 1:DX_CHUNKS + 1 + N_ACC]
    buf, sem, stage, stage_sem = refs[DX_CHUNKS + 1 + N_ACC:]
    n_out, width = out.shape
    seq = buf.shape[1] // SUBL
    part = seq // DX_CHUNKS

    def load(i, h):
        slot = lax.rem(i, 3)
        return pltpu.make_async_copy(rows[h].at[i], buf.at[slot, pl.ds(h * part * SUBL, part * SUBL)], sem.at[slot, h])

    def each_load(i, act):
        low, high = starts[i], starts[i] + counts[i]
        for h in range(DX_CHUNKS):
            @pl.when(jnp.logical_and(low < (h + 1) * part, jnp.logical_and(high > h * part, counts[i] > 0)))
            def _():
                act(load(i, h))

    def launch(copy):
        copy.start()

    def settle(copy):
        copy.wait()

    each_load(0, launch)
    each_load(1, launch)

    @pl.loop(0, n_out)
    def _(r):
        for acc in accs:
            acc[pl.ds(pl.multiple_of(r * SUBL, SUBL), SUBL), :] = jnp.zeros((SUBL, LANES), jnp.float32)

    def add_row(i, k, acc):
        row = pl.multiple_of(ids[i * seq + k] * SUBL, SUBL)
        acc[pl.ds(row, SUBL), :] += buf[lax.rem(i, 3), pl.ds(pl.multiple_of(k * SUBL, SUBL), SUBL), :]

    @pl.loop(0, N_DEV)
    def _(i):
        @pl.when(i + 2 < N_DEV)
        def _():
            each_load(i + 2, launch)
        each_load(i, settle)
        start = starts[i]
        count = counts[i]
        full = lax.div(count, 8)

        @pl.loop(0, full)
        def _(t):
            for u in range(8):
                add_row(i, start + t * 8 + u, accs[u % N_ACC])

        @pl.loop(full * 8, count)
        def _(k):
            add_row(i, start + k, accs[0])

    def store(m):
        here = pl.ds(pl.multiple_of(m * OUT_ROWS, OUT_ROWS), OUT_ROWS)
        return pltpu.make_async_copy(stage.at[lax.rem(m, 2)], out.at[here], stage_sem.at[lax.rem(m, 2)])
    n_store = n_out // OUT_ROWS

    @pl.loop(0, n_store)
    def _(m):
        @pl.when(m >= 2)
        def _():
            store(m - 2).wait()

        @pl.loop(0, OUT_ROWS // SUBL)
        def _(r):
            for j in range(SUBL):
                lanes = min(LANES, width - j * LANES)
                here = pl.ds(m * (OUT_ROWS * SUBL) + r * (SUBL * SUBL) + j, SUBL, stride=SUBL)
                value = accs[0][here, :]
                for acc in accs[1:]:
                    value = value + acc[here, :]
                stage[lax.rem(m, 2), pl.ds(pl.multiple_of(r * SUBL, SUBL), SUBL), pl.ds(j * LANES, lanes)] = value[:, :lanes]
        store(m).start()
    for m in (n_store - 2, n_store - 1):
        store(m).wait()


def add_rows(ids, starts, counts, rows, n_out, width):
    smem = pl.BlockSpec(memory_space=pltpu.SMEM)
    seq_rows = DX_CHUNKS * rows[0].shape[1]
    return pl.pallas_call(
        add_kernel,
        out_shape=jax.ShapeDtypeStruct((n_out, width), jnp.float32),
        in_specs=[smem] * 3 + [pl.BlockSpec(memory_space=pltpu.HBM)] * DX_CHUNKS,
        out_specs=pl.BlockSpec(memory_space=pltpu.HBM),
        scratch_shapes=[pltpu.VMEM((n_out * SUBL, LANES), jnp.float32)] * N_ACC + [
            pltpu.VMEM((3, seq_rows, LANES), jnp.float32), pltpu.SemaphoreType.DMA((3, DX_CHUNKS)),
            pltpu.VMEM((2, OUT_ROWS, width), jnp.float32), pltpu.SemaphoreType.DMA((2,))],
        compiler_params=pltpu.CompilerParams(vmem_limit_bytes=VMEM_BYTES),
        name='add_rows',
    )(ids, starts, counts, *rows)


def rope_tables(positions, head_dim):
    half_dim = head_dim // 2
    inv_freq = jnp.exp(jnp.arange(half_dim, dtype=jnp.float32) * (-2.0 * math.log(ROPE_THETA) / head_dim))
    angles = positions.astype(jnp.float32)[:, None] * inv_freq
    return jnp.cos(angles), jnp.sin(angles)


def rotate(values, cos_t, sin_t):
    half_dim = values.shape[-1] // 2
    lead_half = values[..., :half_dim]
    tail_half = values[..., half_dim:]
    return jnp.concatenate([lead_half * cos_t - tail_half * sin_t, tail_half * cos_t + lead_half * sin_t], axis=-1)


def norm_fwd(values):
    values_f = values.astype(jnp.float32)
    inv_rms = lax.rsqrt(jnp.mean(values_f * values_f, axis=-1, keepdims=True) + NORM_EPS)
    return values_f * inv_rms, inv_rms


def norm_bwd(grad_out, normed, inv_rms, norm_gain):
    grad_normed = grad_out * norm_gain.astype(jnp.float32)
    mean_term = jnp.mean(grad_normed * normed, axis=-1, keepdims=True)
    return inv_rms * (grad_normed - normed * mean_term)


def attn_fwd(q_rot, k_rot, v_raw):
    seq_len = q_rot.shape[0]
    attn_scale = q_rot.shape[-1] ** -0.5
    scores = jnp.einsum('qgrh,kgh->grqk', q_rot, k_rot, preferred_element_type=jnp.float32) * attn_scale
    causal = lax.broadcasted_iota(jnp.int32, (seq_len, seq_len), 0) >= lax.broadcasted_iota(jnp.int32, (seq_len, seq_len), 1)
    attn_probs = jax.nn.softmax(jnp.where(causal, scores, -1e30), axis=-1)
    attn_heads = jnp.einsum('grqk,kgh->qgrh', attn_probs.astype(jnp.bfloat16), v_raw, preferred_element_type=jnp.float32)
    return attn_heads.astype(jnp.bfloat16), attn_probs


def attn_bwd(grad_b, q_rot, k_rot, v_raw, attn_probs):
    attn_scale = q_rot.shape[-1] ** -0.5
    probs_b = attn_probs.astype(jnp.bfloat16)
    grad_probs = jnp.einsum('qgrh,kgh->grqk', grad_b, v_raw, preferred_element_type=jnp.float32)
    grad_v = jnp.einsum('grqk,qgrh->kgh', probs_b, grad_b, preferred_element_type=jnp.float32)
    grad_scores = attn_probs * (grad_probs - jnp.sum(grad_probs * attn_probs, axis=-1, keepdims=True)) * attn_scale
    scores_b = grad_scores.astype(jnp.bfloat16)
    grad_q = jnp.einsum('grqk,kgh->qgrh', scores_b, k_rot, preferred_element_type=jnp.float32)
    grad_k = jnp.einsum('grqk,qgrh->kgh', scores_b, q_rot, preferred_element_type=jnp.float32)
    return grad_q, grad_k, grad_v


def dot_f32(lhs, rhs):
    return jnp.dot(lhs, rhs, preferred_element_type=jnp.float32)


def dot_t(lhs, rhs):
    return lax.dot_general(lhs, rhs, (((0,), (0,)), ((), ())), preferred_element_type=jnp.float32)


def dot_nt(lhs, rhs):
    return lax.dot_general(lhs, rhs, (((1,), (1,)), ((), ())), preferred_element_type=jnp.float32)


def pad_rows(shard, rows):
    return jnp.pad(shard, ((0, rows - shard.shape[0]), (0, 0)))


def solution(mesh):
    row_spec = P(AXIS_NAME, None)
    vec_spec = P(AXIS_NAME)
    full_spec = P(None)
    batch_spec = P(AXIS_NAME, None, None)
    weight_specs = (vec_spec, row_spec, row_spec, row_spec, full_spec, full_spec, row_spec, vec_spec, row_spec, row_spec, row_spec)

    def device_step(tokens, positions, table_shard, attn_norm_s, w_query, w_key, w_value, q_norm, k_norm, w_out, mlp_norm_s, w_gate, w_up, w_down, dy_out):
        me = lax.axis_index(AXIS_NAME)
        seq = tokens.shape[1]
        rows_local, dim = table_shard.shape
        part = dim // N_DEV
        part_p = -(-part // 16) * 16
        dim_p = part_p * N_DEV
        head_dim = q_norm.shape[0]
        n_q = w_query.shape[1]
        n_kv = w_key.shape[1]
        kv_heads = n_kv // head_dim
        q_per_kv = n_q // n_kv

        ids = tokens[0]
        order = jnp.arange(seq, dtype=jnp.int32)
        keys = ids * seq + order
        rank = jnp.sum((keys[None, :] < keys[:, None]).astype(jnp.int32), axis=1)
        sorted_ids = jnp.sum(jnp.where(rank[None, :] == order[:, None], ids[None, :], 0), axis=1)
        all_keys = gather_ids(jnp.concatenate([ids, sorted_ids]).reshape(2 * seq // LANES, LANES)).reshape(N_DEV, 2, seq)
        all_ids = all_keys[:, 0]
        sorted_all = all_keys[:, 1]
        chip_ids = (all_ids - me // NC * (NC * rows_local)).reshape(-1)
        width_p = SUBL * LANES
        table_rows = jnp.pad(table_shard, ((0, 0), (0, width_p - dim))).reshape(rows_local, SUBL, LANES)
        x_emb = fetch_rows(chip_ids, table_rows, seq).reshape(seq, width_p)[:, :dim].astype(jnp.float32)
        low = me * rows_local
        my_starts = jnp.sum((sorted_all < low).astype(jnp.int32), axis=1)
        my_counts = jnp.sum((sorted_all < low + rows_local).astype(jnp.int32), axis=1) - my_starts
        local_ids = jnp.clip(sorted_all - low, 0, rows_local - 1).reshape(-1)

        norm_pad = ((0, 0), (0, LANES - part))
        gains = jnp.concatenate([jnp.pad(attn_norm_s[None], norm_pad), jnp.pad(mlp_norm_s[None], norm_pad), jnp.zeros((14, LANES), attn_norm_s.dtype)], axis=0)
        w_qkv = jnp.concatenate([w_query, w_key, w_value], axis=1)
        blocks = [gains, pad_rows(w_qkv, part_p), pad_rows(w_out, part_p)]
        gains_all, w_qkv_p, w_out_p = gather_blocks(blocks, 0, 1, 'gather_weights')
        w_gate_p, w_up_p, w_down_f = (lax.all_gather(w, AXIS_NAME, tiled=True) for w in (pad_rows(w_gate, part_p), pad_rows(w_up, part_p), w_down))
        attn_norm = gains_all[:, 0, :part].reshape(dim)
        mlp_norm = gains_all[:, 1, :part].reshape(dim)
        w_qkv_p, w_out_p, w_gate_p, w_up_p, w_down_f = (w.reshape(-1, w.shape[-1]) for w in (w_qkv_p, w_out_p, w_gate_p, w_up_p, w_down_f))

        wide_pos = jnp.arange(dim_p, dtype=jnp.int32)
        dim_pos = jnp.arange(dim, dtype=jnp.int32)
        spread = (wide_pos[None, :] == (dim_pos // part * part_p + dim_pos % part)[:, None]).astype(jnp.bfloat16)

        def widen(values):
            return dot_f32(values, spread).astype(jnp.bfloat16)

        def narrow(values):
            return values.reshape(seq, N_DEV, part_p)[:, :, :part].reshape(seq, dim)

        cos_t, sin_t = rope_tables(positions[0], head_dim)
        cos_q, sin_q = cos_t[:, None, None, :], sin_t[:, None, None, :]
        cos_k, sin_k = cos_t[:, None, :], sin_t[:, None, :]
        normed1, norm1_inv = norm_fwd(x_emb)
        attn_in = widen((normed1 * attn_norm.astype(jnp.float32)).astype(jnp.bfloat16))
        qkv = dot_f32(attn_in, w_qkv_p).astype(jnp.bfloat16)
        q_raw = qkv[:, :n_q].reshape(seq, kv_heads, q_per_kv, head_dim)
        k_raw = qkv[:, n_q:n_q + n_kv].reshape(seq, kv_heads, head_dim)
        v_raw = qkv[:, n_q + n_kv:].reshape(seq, kv_heads, head_dim)
        q_normed, q_inv = norm_fwd(q_raw)
        k_normed, k_inv = norm_fwd(k_raw)
        q_rot = rotate(q_normed * q_norm.astype(jnp.float32), cos_q, sin_q).astype(jnp.bfloat16)
        k_rot = rotate(k_normed * k_norm.astype(jnp.float32), cos_k, sin_k).astype(jnp.bfloat16)
        attn_heads, attn_probs = attn_fwd(q_rot, k_rot, v_raw)
        attn_flat = widen(attn_heads.reshape(seq, n_q))
        hidden = (x_emb + dot_f32(attn_flat, w_out_p)).astype(jnp.bfloat16)
        normed2, norm2_inv = norm_fwd(hidden)
        mlp_in = widen((normed2 * mlp_norm.astype(jnp.float32)).astype(jnp.bfloat16))
        gate_pre = dot_f32(mlp_in, w_gate_p)
        up_proj = dot_f32(mlp_in, w_up_p)
        mlp_act = (jax.nn.silu(gate_pre) * up_proj).astype(jnp.bfloat16)
        layer_out = (hidden.astype(jnp.float32) + dot_f32(mlp_act, w_down_f)).astype(jnp.bfloat16)

        dy = dy_out[0]
        grad_w_down = dot_t(mlp_act, dy)
        grad_act = dot_nt(dy, w_down_f)
        gate_sig = jax.nn.sigmoid(gate_pre)
        grad_gate = (grad_act * up_proj * gate_sig * (1.0 + gate_pre * (1.0 - gate_sig))).astype(jnp.bfloat16)
        grad_up = (grad_act * gate_pre * gate_sig).astype(jnp.bfloat16)
        grad_w_gate = dot_t(mlp_in, grad_gate)
        grad_w_up = dot_t(mlp_in, grad_up)
        grad_mlp_in = narrow(dot_nt(grad_gate, w_gate_p) + dot_nt(grad_up, w_up_p))
        grad_mlp_norm = jnp.sum(grad_mlp_in * normed2, axis=0)
        grad_hidden = dy.astype(jnp.float32) + norm_bwd(grad_mlp_in, normed2, norm2_inv, mlp_norm)
        hidden_b = grad_hidden.astype(jnp.bfloat16)
        grad_w_out = dot_t(attn_flat, hidden_b)
        grad_heads = dot_nt(dot_nt(hidden_b, w_out_p).astype(jnp.bfloat16), spread).astype(jnp.bfloat16).reshape(q_rot.shape)
        grad_q, grad_k, grad_v = attn_bwd(grad_heads, q_rot, k_rot, v_raw, attn_probs)
        grad_qt = rotate(grad_q, cos_q, -sin_q)
        grad_kt = rotate(grad_k, cos_k, -sin_k)
        grad_q_norm = jnp.sum(grad_qt * q_normed, axis=(0, 1, 2))
        grad_k_norm = jnp.sum(grad_kt * k_normed, axis=(0, 1))
        grad_q_raw = norm_bwd(grad_qt, q_normed, q_inv, q_norm).astype(jnp.bfloat16).reshape(seq, n_q)
        grad_k_raw = norm_bwd(grad_kt, k_normed, k_inv, k_norm).astype(jnp.bfloat16).reshape(seq, n_kv)
        grad_v_raw = grad_v.astype(jnp.bfloat16).reshape(seq, n_kv)
        grad_qkv = jnp.concatenate([grad_q_raw, grad_k_raw, grad_v_raw], axis=1)
        grad_attn_in = narrow(dot_nt(grad_qkv, w_qkv_p))
        grad_x_emb = grad_hidden + norm_bwd(grad_attn_in, normed1, norm1_inv, attn_norm)
        dx_rows = pack_rows(rank, grad_x_emb)
        dx_all = gather_blocks(dx_rows, 1, 4, 'gather_dx')

        grad_attn_norm = jnp.sum(grad_attn_in * normed1, axis=0)
        grad_w_qkv = dot_t(attn_in, grad_qkv)
        small = jnp.stack([jnp.pad(grad_attn_norm.reshape(N_DEV, part), norm_pad), jnp.pad(grad_mlp_norm.reshape(N_DEV, part), norm_pad),
                           jnp.broadcast_to(jnp.concatenate([grad_q_norm, grad_k_norm])[None], (N_DEV, 2 * head_dim))], axis=1)
        small = jnp.pad(small, ((0, 0), (0, SUBL - 3), (0, 0)))
        parts = [small] + [g.reshape(N_DEV, -1, g.shape[-1]) for g in (grad_w_qkv, grad_w_out, grad_w_gate, grad_w_up,)]
        small_s, qkv_s, out_s, gate_s, up_s = scatter_grads(parts)
        down_s, = (lax.psum_scatter(g, AXIS_NAME, scatter_dimension=0, tiled=True) for g in (grad_w_down,))
        d_table = add_rows(local_ids, my_starts, my_counts, dx_all, rows_local, dim)
        return (layer_out[None], d_table, small_s[0, :part], qkv_s[:part, :n_q], qkv_s[:part, n_q:n_q + n_kv], qkv_s[:part, n_q + n_kv:],
                small_s[2, :head_dim], small_s[2, head_dim:], out_s[:part], small_s[1, :part], gate_s[:part], up_s[:part], down_s)

    return jax.shard_map(device_step, mesh=mesh, in_specs=(row_spec, row_spec, row_spec) + weight_specs + (batch_spec,), out_specs=(batch_spec, row_spec) + weight_specs, check_vma=False)
```

```python
import functools
import math
import jax
import jax.numpy as jnp
from jax import lax
from jax.experimental import pallas as pl
from jax.experimental.pallas import tpu as pltpu
from jax.sharding import PartitionSpec as P

NORM_EPS = 1e-6
ROPE_THETA = 1.0e6
AXIS_NAME = 'fsdp'
MESH = pl.DeviceIdType.MESH
NZ, NQ, NC = 4, 4, 2
N_DEV = NZ * NQ * NC
LANES = 128
SUBL = 8
VMEM_BYTES = 62 * 1024 * 1024
J_GATHER = (0, 1, 3, 2)
J_SCATTER = (2, 1, 3, 0)


def dev_id(z, q, c):
    y = lax.div(q, 2)
    x = lax.rem(q + y, 2)
    return z * 8 + y * 4 + x * 2 + c


def my_coords():
    me = lax.axis_index(AXIS_NAME)
    z = lax.div(me, 8)
    y = lax.rem(lax.div(me, 4), 2)
    x = lax.rem(lax.div(me, 2), 2)
    c = lax.rem(me, 2)
    q = y * 2 + lax.rem(x + y, 2)
    return me, z, q, c


def wrap4(value):
    return lax.rem(value + 16, 4)


def entry_barrier(z, q, c):
    barrier = pltpu.get_barrier_semaphore()
    peers = [dev_id(wrap4(z + k), q, c) for k in (1, 2, 3)]
    peers += [dev_id(z, wrap4(q + 1), c), dev_id(z, wrap4(q + 3), c), dev_id(z, q, 1 - c)]
    for peer in peers:
        pl.semaphore_signal(barrier, inc=1, device_id=(peer,), device_id_type=MESH)
    pl.semaphore_wait(barrier, len(peers))


def ids_kernel(src, dst, loc_sem, send_sem, recv_sem):
    me = lax.axis_index(AXIS_NAME)
    barrier = pltpu.get_barrier_semaphore()

    @pl.loop(1, N_DEV)
    def _(k):
        pl.semaphore_signal(barrier, inc=1, device_id=(lax.rem(me + k, N_DEV),), device_id_type=MESH)
    pl.semaphore_wait(barrier, N_DEV - 1)
    local = pltpu.make_async_copy(src, dst.at[me], loc_sem)
    local.start()

    @pl.loop(1, N_DEV)
    def _(k):
        pltpu.make_async_remote_copy(src_ref=src, dst_ref=dst.at[me], send_sem=send_sem.at[k], recv_sem=recv_sem.at[k],
                                     device_id=(lax.rem(me + k, N_DEV),), device_id_type=MESH).start()
    local.wait()

    @pl.loop(1, N_DEV)
    def _(k):
        copy = pltpu.make_async_remote_copy(src_ref=src, dst_ref=dst.at[lax.rem(me + N_DEV - k, N_DEV)], send_sem=send_sem.at[k],
                                            recv_sem=recv_sem.at[k], device_id=(lax.rem(me + k, N_DEV),), device_id_type=MESH)
        copy.wait_send()
        copy.wait_recv()


def gather_ids(block):
    return pl.pallas_call(
        ids_kernel,
        out_shape=jax.ShapeDtypeStruct((N_DEV,) + block.shape, block.dtype),
        in_specs=[pl.BlockSpec(memory_space=pltpu.VMEM)],
        out_specs=pl.BlockSpec(memory_space=pltpu.VMEM),
        scratch_shapes=[pltpu.SemaphoreType.DMA, pltpu.SemaphoreType.DMA((N_DEV,)), pltpu.SemaphoreType.DMA((N_DEV,))],
        compiler_params=pltpu.CompilerParams(collective_id=0, has_side_effects=True),
        name='gather_ids',
    )(block)


def blocks_kernel(n_a, n_b, cuts, *refs):
    n_arr = n_a + n_b
    stacked = cuts is not None
    if stacked:
        ins = [refs[0].at[pl.ds(first_row, n_rows)] for first_row, n_rows in cuts]
        refs = refs[1:]
    else:
        ins = refs[:n_arr]
        refs = refs[n_arr:]
    if stacked:
        outs = [refs[0].at[:, pl.ds(first_row, n_rows)] for first_row, n_rows in cuts]
        refs = refs[1:]
    else:
        outs = refs[:n_arr]
        refs = refs[n_arr:]
    loc_sem, az_send, az_recv, ar_send, ar_recv, ap_send, ap_recv, bz_send, bz_recv, br_send, br_recv, bp_send, bp_recv = refs
    me, z, q, c = my_coords()
    step_dir = 1 - 2 * c
    nxt = dev_id(z, wrap4(q + step_dir), c)
    mate = dev_id(z, q, 1 - c)
    high = lax.div(z, 2)
    inner = lax.div(wrap4(z + 1), 2)
    entry_barrier(z, q, c)

    def remote(src, dst, send, recv, target):
        return pltpu.make_async_remote_copy(src_ref=src, dst_ref=dst, send_sem=send, recv_sem=recv, device_id=(target,), device_id_type=MESH)

    def source_z(t):
        if t == 0:
            return z
        base = t - inner if t == 1 else t
        return base + high * (3 - 2 * base)

    def block_at(t, s):
        return dev_id(source_z(t), wrap4(q - step_dir * s), c)

    def spot(a, t, s):
        return outs[a].at[block_at(t, s)]

    def source(a, t, s):
        return ins[a] if (t, s) == (0, 0) else spot(a, t, s)

    def ring(a, t, s):
        if a < n_a:
            sems = ar_send.at[a, s, t], ar_recv.at[a, s, t]
        else:
            sems = br_send.at[a - n_a, s], br_recv.at[a - n_a, s]
        return remote(source(a, t, s), spot(a, t, s), *sems, nxt)

    def ring_in(a, t, s):
        if a < n_a:
            sems = ar_send.at[a, s, t], ar_recv.at[a, s, t]
        else:
            sems = br_send.at[a - n_a, s], br_recv.at[a - n_a, s]
        return remote(spot(a, t, s + 1), spot(a, t, s + 1), *sems, nxt)

    def pair_sems(a, t, s):
        if a < n_a:
            return ap_send.at[a, s, t], ap_recv.at[a, s, t]
        return bp_send.at[a - n_a, s, t], bp_recv.at[a - n_a, s, t]

    def pair(a, t, s):
        return remote(source(a, t, s), spot(a, t, s), *pair_sems(a, t, s), mate)

    def pair_in(a, t, s):
        dst = outs[a].at[dev_id(source_z(t), wrap4(q + step_dir * s), 1 - c)]
        return remote(dst, dst, *pair_sems(a, t, s), mate)

    def column(a, t, s, up):
        side = 0 if up else 1
        if a < n_a:
            sems = az_send.at[a, side, t], az_recv.at[a, source_z(t)]
        else:
            sems = bz_send.at[a - n_a, s, side, t], bz_recv.at[a - n_a, s, source_z(t)]
        return remote(source(a, t, s), spot(a, t, s), *sems, dev_id(z + 1 if up else z - 1, q, c))

    def column_in(a, t, s):
        if a < n_a:
            sems = az_send.at[a, 0, t], az_recv.at[a, source_z(t)]
        else:
            sems = bz_send.at[a - n_a, s, 0, t], bz_recv.at[a - n_a, s, source_z(t)]
        return remote(spot(a, t, s), spot(a, t, s), *sems, mate)

    def spread(a, t, s, act):
        if t == 0:
            ups, downs = z < NZ - 1, z > 0
        else:
            ups = jnp.logical_and(inner == 1, source_z(t) < z)
            downs = jnp.logical_and(inner == 1, source_z(t) > z)

        @pl.when(ups)
        def _():
            act(column(a, t, s, True))

        @pl.when(downs)
        def _():
            act(column(a, t, s, False))

    def launch(copy):
        copy.start()

    def settle(copy):
        copy.wait_send()

    first = range(n_a)
    second = range(n_a, n_arr)
    local = [pltpu.make_async_copy(ins[a], outs[a].at[me], loc_sem.at[a]) for a in range(n_arr)]
    for a in list(second) + list(first):
        ring(a, 0, 0).start()
    for a in range(n_arr):
        spread(a, 0, 0, launch)
    for a in range(n_arr):
        local[a].start()
        pair(a, 0, 0).start()

    def ring_step(a, t, s):
        ring_in(a, t, s - 1).wait_recv()
        if s < 3:
            ring(a, t, s).start()
        pair(a, t, s).start()

    groups = []
    for t in range(NZ):
        groups += [(t, 1), (t, 2)]
        if t + 1 < NZ:
            groups.append((t + 1, 0))
        groups.append((t, 3))
    later = [(t, s) for t in (1, 2, 3) for s in range(4)]
    for t, s in groups:
        for a in first:
            if s == 0:
                column_in(a, t, 0).wait_recv()
                ring(a, t, 0).start()
                spread(a, t, 0, launch)
                pair(a, t, 0).start()
            else:
                ring_step(a, t, s)
        for a in second:
            if t == 0 and s > 0:
                ring_step(a, 0, s)
                spread(a, 0, s, launch)
            if (t, s) in ((0, 1), (0, 2)) or not later:
                continue
            tb, sb = later[0]
            if tb == 1 and sb == 3 and (t, s) == (1, 0):
                continue
            column_in(a, tb, sb).wait_recv()
            spread(a, tb, sb, launch)
            pair(a, tb, sb).start()
        if (t, s) not in ((0, 1), (0, 2)) and later:
            later.pop(0)
    for tb, sb in later:
        for a in second:
            column_in(a, tb, sb).wait_recv()
            spread(a, tb, sb, launch)
            pair(a, tb, sb).start()
    for a in range(n_arr):
        local[a].wait()
        for t in range(NZ):
            for s in range(4):
                pair_in(a, t, s).wait_recv()
                pair(a, t, s).wait_send()
                if s < 3 and (a < n_a or t == 0):
                    ring(a, t, s).wait_send()
                if s == 0 or a >= n_a:
                    spread(a, t, s, settle)


def gather_blocks(blocks, n_b, collective_id, name, cuts=None):
    stacked = cuts is not None
    n_arr = len(cuts) if stacked else len(blocks)
    n_a = n_arr - n_b
    n_b1 = max(n_b, 1)
    out_shape = tuple(jax.ShapeDtypeStruct((N_DEV,) + b.shape, b.dtype) for b in ([blocks] if stacked else blocks))
    dma = pltpu.SemaphoreType.DMA
    operands = [blocks] if stacked else blocks
    return pl.pallas_call(
        functools.partial(blocks_kernel, n_a, n_b, cuts),
        out_shape=out_shape,
        in_specs=[pl.BlockSpec(memory_space=pltpu.VMEM)] * len(operands),
        out_specs=tuple(pl.BlockSpec(memory_space=pltpu.HBM) for _ in out_shape),
        scratch_shapes=[dma((n_arr,)), dma((n_a, 2, 4)), dma((n_a, 4)), dma((n_a, 3, 4)), dma((n_a, 3, 4)), dma((n_a, 4, 4)), dma((n_a, 4, 4)),
                        dma((n_b1, 4, 2, 4)), dma((n_b1, 4, 4)), dma((n_b1, 3)), dma((n_b1, 3)), dma((n_b1, 4, 4)), dma((n_b1, 4, 4))],
        compiler_params=pltpu.CompilerParams(collective_id=collective_id, has_side_effects=True, vmem_limit_bytes=8 * 1024 * 1024),
        name=name,
    )(*operands)


N_GROUPS = 16


def grads_kernel(n_arr, *refs):
    ins = refs[:n_arr]
    outs = refs[n_arr:2 * n_arr]
    scratch = refs[2 * n_arr:]
    own, mbuf, rbuf, zbuf = (scratch[i * n_arr:(i + 1) * n_arr] for i in range(4))
    o_sem, z_send, z_recv, r_send, r_recv, p_send, p_recv = scratch[4 * n_arr:]
    me, z, q, c = my_coords()
    step_dir = 1 - 2 * c
    nxt = dev_id(z, wrap4(q + step_dir), c)
    mate = dev_id(z, q, 1 - c)
    arrays = range(n_arr)
    groups = []
    for pos, j in enumerate(J_SCATTER):
        if pos == 0:
            groups.append((j, 0))
        groups += [(j, 1), (j, 2)]
        if pos + 1 < NZ:
            groups.append((J_SCATTER[pos + 1], 0))
        groups.append((j, 3))
    n_groups = len(groups)

    def remote(src, dst, send, recv, target):
        return pltpu.make_async_remote_copy(src_ref=src, dst_ref=dst, send_sem=send, recv_sem=recv, device_id=(target,), device_id_type=MESH)

    def own_load(g, a):
        j, s = groups[g]
        block = dev_id(wrap4(z + j), wrap4(q - step_dir * (1 + s)), c)
        return pltpu.make_async_copy(ins[a].at[block], own[a].at[g % 2], o_sem.at[a, g % 2])

    def pair(g, a):
        j, s = groups[g]
        block = dev_id(wrap4(z + j), wrap4(q + step_dir * (1 + s)), 1 - c)
        return remote(ins[a].at[block], mbuf[a].at[g], p_send.at[a, g], p_recv.at[a, g], mate)

    def place(j, s):
        return j * 3 + s

    def ring(g, a):
        j, s = groups[g]
        src = mbuf[a].at[g] if s == 0 else rbuf[a].at[place(j, s - 1)]
        return remote(src, rbuf[a].at[place(j, s)], r_send.at[a, place(j, s)], r_recv.at[a, place(j, s)], nxt)

    def column(a, j):
        return remote(rbuf[a].at[place(j, 2)], zbuf[a].at[j - 1], z_send.at[a, j - 1], z_recv.at[a, j - 1], dev_id(wrap4(z + j), q, c))

    def add_into(dst, others):
        rows = dst.shape[0]

        @pl.loop(0, rows // SUBL)
        def _(r):
            here = pl.ds(pl.multiple_of(r * SUBL, SUBL), SUBL)
            total = dst[here, :]
            for other in others:
                total = total + other[here, :]
            dst[here, :] = total

    for a in arrays:
        own_load(0, a).start()
    entry_barrier(z, q, c)
    for g in range(3):
        for a in arrays:
            pair(g, a).start()
    for g, (j, s) in enumerate(groups):
        for a in arrays:
            if g + 1 < n_groups:
                own_load(g + 1, a).start()
            if g + 3 < n_groups:
                pair(g + 3, a).start()
        for a in arrays:
            own_load(g, a).wait()
            pair(g, a).wait_recv()
            if s == 0:
                add_into(mbuf[a].at[g], [own[a].at[g % 2]])
            else:
                slot = place(j, s - 1)
                remote(rbuf[a].at[slot], rbuf[a].at[slot], r_send.at[a, slot], r_recv.at[a, slot], nxt).wait_recv()
                add_into(rbuf[a].at[slot], [own[a].at[g % 2], mbuf[a].at[g]])
            if s < 3:
                ring(g, a).start()
            elif j != 0:
                column(a, j).start()
    for a in arrays:
        for j in (1, 2, 3):
            column(a, j).wait_recv()
        rows = outs[a].shape[0]

        @pl.loop(0, rows // SUBL)
        def _(r):
            here = pl.ds(pl.multiple_of(r * SUBL, SUBL), SUBL)
            total = rbuf[a][place(0, 2), here, :]
            for k in range(3):
                total = total + zbuf[a][k, here, :]
            outs[a][here, :] = total
    for a in arrays:
        for g, (j, s) in enumerate(groups):
            pair(g, a).wait_send()
            if s < 3:
                ring(g, a).wait_send()
        for j in (1, 2, 3):
            column(a, j).wait_send()


def scatter_grads(parts):
    n_arr = len(parts)
    shapes = [p.shape[1:] for p in parts]
    dma = pltpu.SemaphoreType.DMA

    def bufs(count):
        return [pltpu.VMEM((count,) + s, jnp.float32) for s in shapes]

    return pl.pallas_call(
        functools.partial(grads_kernel, n_arr),
        out_shape=tuple(jax.ShapeDtypeStruct(s, jnp.float32) for s in shapes),
        in_specs=[pl.BlockSpec(memory_space=pltpu.HBM)] * n_arr,
        out_specs=tuple(pl.BlockSpec(memory_space=pltpu.VMEM) for _ in parts),
        scratch_shapes=bufs(2) + bufs(16) + bufs(12) + bufs(3) + [
            dma((n_arr, 2)), dma((n_arr, 3)), dma((n_arr, 3)), dma((n_arr, 12)), dma((n_arr, 12)), dma((n_arr, 16)), dma((n_arr, 16))],
        compiler_params=pltpu.CompilerParams(collective_id=2, has_side_effects=True, vmem_limit_bytes=VMEM_BYTES),
        name='scatter_grads',
    )(*parts)


X_CHUNKS = 4


def rows_kernel(ids, table, out, tab, first, rbuf, zbuf, loc_sem, t_send, t_recv, z_send, z_recv, r_send, r_recv):
    me, z, q, c = my_coords()
    step_dir = 1 - 2 * c
    nxt = dev_id(z, wrap4(q + step_dir), c)
    mate = dev_id(z, q, 1 - c)
    n_local = table.shape[0]
    seq = out.shape[0]
    step = seq // X_CHUNKS
    groups = []
    for pos, j in enumerate(J_SCATTER):
        if pos == 0:
            groups.append((j, 0))
        groups += [(j, 1), (j, 2)]
        if pos + 1 < NZ:
            groups.append((J_SCATTER[pos + 1], 0))
        groups.append((j, 3))

    def remote(src, dst, send, recv, target):
        return pltpu.make_async_remote_copy(src_ref=src, dst_ref=dst, send_sem=send, recv_sem=recv, device_id=(target,), device_id_type=MESH)

    mine = tab.at[pl.ds(c * n_local, n_local)]
    local = pltpu.make_async_copy(table, mine, loc_sem)
    local.start()
    entry_barrier(z, q, c)
    share = remote(table, mine, t_send, t_recv, mate)
    share.start()
    local.wait()
    theirs = tab.at[pl.ds((1 - c) * n_local, n_local)]
    remote(table, theirs, t_send, t_recv, mate).wait_recv()

    def place(j, s):
        return j * 3 + s

    def part(ref, h):
        return ref.at[pl.ds(h * step, step)]

    def ring(j, s, h):
        src = first.at[j] if s == 0 else rbuf.at[place(j, s - 1)]
        return remote(part(src, h), part(rbuf.at[place(j, s)], h), r_send.at[place(j, s), h], r_recv.at[place(j, s), h], nxt)

    def column(j, h):
        return remote(part(rbuf.at[place(j, 2)], h), part(zbuf.at[j - 1], h), z_send.at[j - 1, h], z_recv.at[j - 1, h], dev_id(wrap4(z + j), q, c))

    for j, s in groups:
        block = dev_id(wrap4(z + j), wrap4(q - step_dir * (1 + s)), c)
        for h in range(X_CHUNKS):
            if s > 0:
                slot = place(j, s - 1)
                landed = part(rbuf.at[slot], h)
                remote(landed, landed, r_send.at[slot, h], r_recv.at[slot, h], nxt).wait_recv()
                dst = rbuf.at[slot]
            else:
                dst = first.at[j]

            @pl.loop(0, step // SUBL)
            def _(t):
                for u in range(SUBL):
                    k = h * step + t * SUBL + u
                    row = ids[block * seq + k]
                    held = jnp.logical_and(row >= 0, row < 2 * n_local)
                    value = tab[jnp.clip(row, 0, 2 * n_local - 1)]
                    base = jnp.zeros_like(value) if s == 0 else dst[k]
                    dst[k] = jnp.where(held, value, base)
            if s < 3:
                ring(j, s, h).start()
            elif j != 0:
                column(j, h).start()
    for h in range(X_CHUNKS):
        for j in (1, 2, 3):
            column(j, h).wait_recv()

        @pl.loop(0, step // SUBL)
        def _(t):
            here = pl.ds(h * step + t * SUBL, SUBL)
            total = rbuf[place(0, 2), here]
            for k in range(3):
                total = total + zbuf[k, here]
            out[here] = total
    for h in range(X_CHUNKS):
        for j in range(NZ):
            for s in range(3):
                ring(j, s, h).wait_send()
        for j in (1, 2, 3):
            column(j, h).wait_send()
    share.wait_send()


def fetch_rows(ids, table, seq):
    row = table.shape[1:]
    dma = pltpu.SemaphoreType.DMA
    vmem = pl.BlockSpec(memory_space=pltpu.VMEM)
    return pl.pallas_call(
        rows_kernel,
        out_shape=jax.ShapeDtypeStruct((seq,) + row, table.dtype),
        in_specs=[pl.BlockSpec(memory_space=pltpu.SMEM), vmem],
        out_specs=vmem,
        scratch_shapes=[pltpu.VMEM((2 * table.shape[0],) + row, table.dtype), pltpu.VMEM((4, seq) + row, table.dtype), pltpu.VMEM((12, seq) + row, table.dtype),
                        pltpu.VMEM((3, seq) + row, table.dtype), dma, dma, dma, dma((3, X_CHUNKS)), dma((3, X_CHUNKS)), dma((12, X_CHUNKS)), dma((12, X_CHUNKS))],
        compiler_params=pltpu.CompilerParams(collective_id=3, has_side_effects=True, vmem_limit_bytes=48 * 1024 * 1024),
        name='fetch_rows',
    )(ids, table)


N_ACC = 4
DX_CHUNKS = 4
DX_CUTS = (144, 136, 136, 96)


def pack_kernel(rank, dx, out, tmp):
    seq, width = dx.shape

    @pl.loop(0, seq // SUBL)
    def _(r):
        here = pl.ds(pl.multiple_of(r * SUBL, SUBL), SUBL)
        for j in range(SUBL):
            lanes = min(LANES, width - j * LANES)
            value = dx[here, pl.ds(j * LANES, lanes)]
            if lanes < LANES:
                value = jnp.concatenate([value, jnp.zeros((SUBL, LANES - lanes), value.dtype)], axis=1)
            tmp[pl.ds(r * (SUBL * SUBL) + j, SUBL, stride=SUBL), :] = value

    @pl.loop(0, seq // SUBL)
    def _(r):
        for u in range(SUBL):
            i = r * SUBL + u
            row = pl.multiple_of(rank[i] * SUBL, SUBL)
            out[pl.ds(row, SUBL), :] = tmp[pl.ds(pl.multiple_of(i * SUBL, SUBL), SUBL), :]


def pack_rows(rank, dx):
    seq = dx.shape[0]
    vmem = pl.BlockSpec(memory_space=pltpu.VMEM)
    return pl.pallas_call(
        pack_kernel,
        out_shape=jax.ShapeDtypeStruct((seq * SUBL, LANES), dx.dtype),
        in_specs=[pl.BlockSpec(memory_space=pltpu.SMEM), vmem],
        out_specs=vmem,
        scratch_shapes=[pltpu.VMEM((seq * SUBL, LANES), dx.dtype)],
        compiler_params=pltpu.CompilerParams(vmem_limit_bytes=16 * 1024 * 1024),
        name='pack_rows',
    )(rank, dx)


OUT_ROWS = 128


def add_kernel(ids, starts, counts, rows, out, *refs):
    accs = refs[:N_ACC]
    buf, sem, stage, stage_sem = refs[N_ACC:]
    width, n_out = out.shape
    seq = buf.shape[1] // SUBL
    part = seq // DX_CHUNKS

    def load(i, h):
        slot = lax.rem(i, 3)
        return pltpu.make_async_copy(rows.at[i, pl.ds(h * part * SUBL, part * SUBL)], buf.at[slot, pl.ds(h * part * SUBL, part * SUBL)], sem.at[slot, h])

    def each_load(i, act):
        low, high = starts[i], starts[i] + counts[i]
        for h in range(DX_CHUNKS):
            @pl.when(jnp.logical_and(low < (h + 1) * part, jnp.logical_and(high > h * part, counts[i] > 0)))
            def _():
                act(load(i, h))

    def launch(copy):
        copy.start()

    def settle(copy):
        copy.wait()

    each_load(0, launch)
    each_load(1, launch)

    @pl.loop(0, n_out)
    def _(r):
        for acc in accs:
            acc[pl.ds(pl.multiple_of(r * SUBL, SUBL), SUBL), :] = jnp.zeros((SUBL, LANES), jnp.float32)

    def add_row(i, k, acc):
        row = pl.multiple_of(ids[i * seq + k] * SUBL, SUBL)
        acc[pl.ds(row, SUBL), :] += buf[lax.rem(i, 3), pl.ds(pl.multiple_of(k * SUBL, SUBL), SUBL), :]

    @pl.loop(0, N_DEV)
    def _(i):
        @pl.when(i + 2 < N_DEV)
        def _():
            each_load(i + 2, launch)
        each_load(i, settle)
        start = starts[i]
        count = counts[i]
        full = lax.div(count, 8)

        @pl.loop(0, full)
        def _(t):
            for u in range(8):
                add_row(i, start + t * 8 + u, accs[u % N_ACC])

        @pl.loop(full * 8, count)
        def _(k):
            add_row(i, start + k, accs[0])

    def store(m):
        here = pl.ds(pl.multiple_of(m * OUT_ROWS, OUT_ROWS), OUT_ROWS)
        return pltpu.make_async_copy(stage.at[lax.rem(m, 2)], out.at[:, here], stage_sem.at[lax.rem(m, 2)])
    n_store = n_out // OUT_ROWS

    @pl.loop(0, n_store)
    def _(m):
        @pl.when(m >= 2)
        def _():
            store(m - 2).wait()
        for j in range(SUBL):
            lanes = min(LANES, width - j * LANES)
            pieces = []
            for r in range(OUT_ROWS // SUBL):
                here = pl.ds(m * (OUT_ROWS * SUBL) + r * (SUBL * SUBL) + j, SUBL, stride=SUBL)
                value = accs[0][here, :]
                for acc in accs[1:]:
                    value = value + acc[here, :]
                pieces.append(value)
            flipped = jnp.concatenate(pieces, axis=0).T
            stage[lax.rem(m, 2), pl.ds(j * LANES, lanes), :] = flipped[:lanes]
        store(m).start()
    for m in (n_store - 2, n_store - 1):
        store(m).wait()


def add_rows(ids, starts, counts, rows, n_out, width):
    smem = pl.BlockSpec(memory_space=pltpu.SMEM)
    seq_rows = rows.shape[1]
    return pl.pallas_call(
        add_kernel,
        out_shape=jax.ShapeDtypeStruct((width, n_out), jnp.float32),
        in_specs=[smem] * 3 + [pl.BlockSpec(memory_space=pltpu.HBM)],
        out_specs=pl.BlockSpec(memory_space=pltpu.HBM),
        scratch_shapes=[pltpu.VMEM((n_out * SUBL, LANES), jnp.float32)] * N_ACC + [
            pltpu.VMEM((3, seq_rows, LANES), jnp.float32), pltpu.SemaphoreType.DMA((3, DX_CHUNKS)),
            pltpu.VMEM((2, width, OUT_ROWS), jnp.float32), pltpu.SemaphoreType.DMA((2,))],
        compiler_params=pltpu.CompilerParams(vmem_limit_bytes=VMEM_BYTES),
        name='add_rows',
    )(ids, starts, counts, rows).T


def rope_tables(positions, head_dim):
    half_dim = head_dim // 2
    inv_freq = jnp.exp(jnp.arange(half_dim, dtype=jnp.float32) * (-2.0 * math.log(ROPE_THETA) / head_dim))
    angles = positions.astype(jnp.float32)[:, None] * inv_freq
    return jnp.cos(angles), jnp.sin(angles)


def rotate(values, cos_t, sin_t):
    half_dim = values.shape[-1] // 2
    lead_half = values[..., :half_dim]
    tail_half = values[..., half_dim:]
    return jnp.concatenate([lead_half * cos_t - tail_half * sin_t, tail_half * cos_t + lead_half * sin_t], axis=-1)


def norm_fwd(values):
    values_f = values.astype(jnp.float32)
    inv_rms = lax.rsqrt(jnp.mean(values_f * values_f, axis=-1, keepdims=True) + NORM_EPS)
    return values_f * inv_rms, inv_rms


def norm_bwd(grad_out, normed, inv_rms, norm_gain):
    grad_normed = grad_out * norm_gain.astype(jnp.float32)
    mean_term = jnp.mean(grad_normed * normed, axis=-1, keepdims=True)
    return inv_rms * (grad_normed - normed * mean_term)


def attn_fwd(q_rot, k_rot, v_raw):
    seq_len = q_rot.shape[0]
    attn_scale = q_rot.shape[-1] ** -0.5
    scores = jnp.einsum('qgrh,kgh->grqk', q_rot, k_rot, preferred_element_type=jnp.float32) * attn_scale
    causal = lax.broadcasted_iota(jnp.int32, (seq_len, seq_len), 0) >= lax.broadcasted_iota(jnp.int32, (seq_len, seq_len), 1)
    attn_probs = jax.nn.softmax(jnp.where(causal, scores, -1e30), axis=-1)
    attn_heads = jnp.einsum('grqk,kgh->qgrh', attn_probs.astype(jnp.bfloat16), v_raw, preferred_element_type=jnp.float32)
    return attn_heads.astype(jnp.bfloat16), attn_probs


def attn_bwd(grad_b, q_rot, k_rot, v_raw, attn_probs):
    attn_scale = q_rot.shape[-1] ** -0.5
    probs_b = attn_probs.astype(jnp.bfloat16)
    grad_probs = jnp.einsum('qgrh,kgh->grqk', grad_b, v_raw, preferred_element_type=jnp.float32)
    grad_v = jnp.einsum('grqk,qgrh->kgh', probs_b, grad_b, preferred_element_type=jnp.float32)
    grad_scores = attn_probs * (grad_probs - jnp.sum(grad_probs * attn_probs, axis=-1, keepdims=True)) * attn_scale
    scores_b = grad_scores.astype(jnp.bfloat16)
    grad_q = jnp.einsum('grqk,kgh->qgrh', scores_b, k_rot, preferred_element_type=jnp.float32)
    grad_k = jnp.einsum('grqk,qgrh->kgh', scores_b, q_rot, preferred_element_type=jnp.float32)
    return grad_q, grad_k, grad_v


def dot_f32(lhs, rhs):
    return jnp.dot(lhs, rhs, preferred_element_type=jnp.float32)


def dot_t(lhs, rhs):
    return lax.dot_general(lhs, rhs, (((0,), (0,)), ((), ())), preferred_element_type=jnp.float32)


def dot_nt(lhs, rhs):
    return lax.dot_general(lhs, rhs, (((1,), (1,)), ((), ())), preferred_element_type=jnp.float32)


def pad_rows(shard, rows):
    return jnp.pad(shard, ((0, rows - shard.shape[0]), (0, 0)))


def solution(mesh):
    row_spec = P(AXIS_NAME, None)
    vec_spec = P(AXIS_NAME)
    full_spec = P(None)
    batch_spec = P(AXIS_NAME, None, None)
    weight_specs = (vec_spec, row_spec, row_spec, row_spec, full_spec, full_spec, row_spec, vec_spec, row_spec, row_spec, row_spec)

    def device_step(tokens, positions, table_shard, attn_norm_s, w_query, w_key, w_value, q_norm, k_norm, w_out, mlp_norm_s, w_gate, w_up, w_down, dy_out):
        me = lax.axis_index(AXIS_NAME)
        seq = tokens.shape[1]
        rows_local, dim = table_shard.shape
        part = dim // N_DEV
        part_p = -(-part // 16) * 16
        dim_p = part_p * N_DEV
        head_dim = q_norm.shape[0]
        n_q = w_query.shape[1]
        n_kv = w_key.shape[1]
        kv_heads = n_kv // head_dim
        q_per_kv = n_q // n_kv

        ids = tokens[0]
        order = jnp.arange(seq, dtype=jnp.int32)
        keys = ids * seq + order
        rank = jnp.sum((keys[None, :] < keys[:, None]).astype(jnp.int32), axis=1)
        sorted_ids = jnp.sum(jnp.where(rank[None, :] == order[:, None], ids[None, :], 0), axis=1)
        all_keys = gather_ids(jnp.concatenate([ids, sorted_ids]).reshape(2 * seq // LANES, LANES)).reshape(N_DEV, 2, seq)
        all_ids = all_keys[:, 0]
        sorted_all = all_keys[:, 1]
        chip_ids = (all_ids - me // NC * (NC * rows_local)).reshape(-1)
        width_p = SUBL * LANES
        table_rows = jnp.pad(table_shard, ((0, 0), (0, width_p - dim))).reshape(rows_local, SUBL, LANES)
        x_emb = fetch_rows(chip_ids, table_rows, seq).reshape(seq, width_p)[:, :dim].astype(jnp.float32)
        low = me * rows_local
        my_starts = jnp.sum((sorted_all < low).astype(jnp.int32), axis=1)
        my_counts = jnp.sum((sorted_all < low + rows_local).astype(jnp.int32), axis=1) - my_starts
        local_ids = jnp.clip(sorted_all - low, 0, rows_local - 1).reshape(-1)

        norm_pad = ((0, 0), (0, LANES - part))
        gains = jnp.concatenate([jnp.pad(attn_norm_s[None], norm_pad), jnp.pad(mlp_norm_s[None], norm_pad), jnp.zeros((14, LANES), attn_norm_s.dtype)], axis=0)
        w_qkv = jnp.concatenate([w_query, w_key, w_value], axis=1)
        blocks = [gains, pad_rows(w_qkv, part_p), pad_rows(w_out, part_p)]
        gains_all, w_qkv_p, w_out_p = gather_blocks(blocks, 0, 1, 'gather_weights')
        w_gate_p, w_up_p, w_down_f = (lax.all_gather(w, AXIS_NAME, tiled=True) for w in (pad_rows(w_gate, part_p), pad_rows(w_up, part_p), w_down))
        attn_norm = gains_all[:, 0, :part].reshape(dim)
        mlp_norm = gains_all[:, 1, :part].reshape(dim)
        w_qkv_p, w_out_p, w_gate_p, w_up_p, w_down_f = (w.reshape(-1, w.shape[-1]) for w in (w_qkv_p, w_out_p, w_gate_p, w_up_p, w_down_f))

        wide_pos = jnp.arange(dim_p, dtype=jnp.int32)
        dim_pos = jnp.arange(dim, dtype=jnp.int32)
        spread = (wide_pos[None, :] == (dim_pos // part * part_p + dim_pos % part)[:, None]).astype(jnp.bfloat16)

        def widen(values):
            return dot_f32(values, spread).astype(jnp.bfloat16)

        def narrow(values):
            return values.reshape(seq, N_DEV, part_p)[:, :, :part].reshape(seq, dim)

        cos_t, sin_t = rope_tables(positions[0], head_dim)
        cos_q, sin_q = cos_t[:, None, None, :], sin_t[:, None, None, :]
        cos_k, sin_k = cos_t[:, None, :], sin_t[:, None, :]
        normed1, norm1_inv = norm_fwd(x_emb)
        attn_in = widen((normed1 * attn_norm.astype(jnp.float32)).astype(jnp.bfloat16))
        qkv = dot_f32(attn_in, w_qkv_p).astype(jnp.bfloat16)
        q_raw = qkv[:, :n_q].reshape(seq, kv_heads, q_per_kv, head_dim)
        k_raw = qkv[:, n_q:n_q + n_kv].reshape(seq, kv_heads, head_dim)
        v_raw = qkv[:, n_q + n_kv:].reshape(seq, kv_heads, head_dim)
        q_normed, q_inv = norm_fwd(q_raw)
        k_normed, k_inv = norm_fwd(k_raw)
        q_rot = rotate(q_normed * q_norm.astype(jnp.float32), cos_q, sin_q).astype(jnp.bfloat16)
        k_rot = rotate(k_normed * k_norm.astype(jnp.float32), cos_k, sin_k).astype(jnp.bfloat16)
        attn_heads, attn_probs = attn_fwd(q_rot, k_rot, v_raw)
        attn_flat = widen(attn_heads.reshape(seq, n_q))
        hidden = (x_emb + dot_f32(attn_flat, w_out_p)).astype(jnp.bfloat16)
        normed2, norm2_inv = norm_fwd(hidden)
        mlp_in = widen((normed2 * mlp_norm.astype(jnp.float32)).astype(jnp.bfloat16))
        gate_pre = dot_f32(mlp_in, w_gate_p)
        up_proj = dot_f32(mlp_in, w_up_p)
        mlp_act = (jax.nn.silu(gate_pre) * up_proj).astype(jnp.bfloat16)
        layer_out = (hidden.astype(jnp.float32) + dot_f32(mlp_act, w_down_f)).astype(jnp.bfloat16)

        dy = dy_out[0]
        grad_w_down = dot_t(mlp_act, dy)
        grad_act = dot_nt(dy, w_down_f)
        gate_sig = jax.nn.sigmoid(gate_pre)
        grad_gate = (grad_act * up_proj * gate_sig * (1.0 + gate_pre * (1.0 - gate_sig))).astype(jnp.bfloat16)
        grad_up = (grad_act * gate_pre * gate_sig).astype(jnp.bfloat16)
        grad_w_gate = dot_t(mlp_in, grad_gate)
        grad_w_up = dot_t(mlp_in, grad_up)
        grad_mlp_in = narrow(dot_nt(grad_gate, w_gate_p) + dot_nt(grad_up, w_up_p))
        grad_mlp_norm = jnp.sum(grad_mlp_in * normed2, axis=0)
        grad_hidden = dy.astype(jnp.float32) + norm_bwd(grad_mlp_in, normed2, norm2_inv, mlp_norm)
        hidden_b = grad_hidden.astype(jnp.bfloat16)
        grad_w_out = dot_t(attn_flat, hidden_b)
        grad_heads = dot_nt(dot_nt(hidden_b, w_out_p).astype(jnp.bfloat16), spread).astype(jnp.bfloat16).reshape(q_rot.shape)
        grad_q, grad_k, grad_v = attn_bwd(grad_heads, q_rot, k_rot, v_raw, attn_probs)
        grad_qt = rotate(grad_q, cos_q, -sin_q)
        grad_kt = rotate(grad_k, cos_k, -sin_k)
        grad_q_norm = jnp.sum(grad_qt * q_normed, axis=(0, 1, 2))
        grad_k_norm = jnp.sum(grad_kt * k_normed, axis=(0, 1))
        grad_q_raw = norm_bwd(grad_qt, q_normed, q_inv, q_norm).astype(jnp.bfloat16).reshape(seq, n_q)
        grad_k_raw = norm_bwd(grad_kt, k_normed, k_inv, k_norm).astype(jnp.bfloat16).reshape(seq, n_kv)
        grad_v_raw = grad_v.astype(jnp.bfloat16).reshape(seq, n_kv)
        grad_qkv = jnp.concatenate([grad_q_raw, grad_k_raw, grad_v_raw], axis=1)
        grad_attn_in = narrow(dot_nt(grad_qkv, w_qkv_p))
        grad_x_emb = grad_hidden + norm_bwd(grad_attn_in, normed1, norm1_inv, attn_norm)
        dx_rows = pack_rows(rank, grad_x_emb)
        cuts = [(SUBL * sum(DX_CUTS[:h]), SUBL * DX_CUTS[h]) for h in range(len(DX_CUTS))]
        dx_all, = gather_blocks(dx_rows, 1, 4, 'gather_dx', cuts)

        grad_attn_norm = jnp.sum(grad_attn_in * normed1, axis=0)
        grad_w_qkv = dot_t(attn_in, grad_qkv)
        small = jnp.stack([jnp.pad(grad_attn_norm.reshape(N_DEV, part), norm_pad), jnp.pad(grad_mlp_norm.reshape(N_DEV, part), norm_pad),
                           jnp.broadcast_to(jnp.concatenate([grad_q_norm, grad_k_norm])[None], (N_DEV, 2 * head_dim))], axis=1)
        small = jnp.pad(small, ((0, 0), (0, SUBL - 3), (0, 0)))
        parts = [small] + [g.reshape(N_DEV, -1, g.shape[-1]) for g in (grad_w_qkv, grad_w_out, grad_w_gate, grad_w_up,)]
        small_s, qkv_s, out_s, gate_s, up_s = scatter_grads(parts)
        down_s, = (lax.psum_scatter(g, AXIS_NAME, scatter_dimension=0, tiled=True) for g in (grad_w_down,))
        d_table = add_rows(local_ids, my_starts, my_counts, dx_all, rows_local, dim)
        return (layer_out[None], d_table, small_s[0, :part], qkv_s[:part, :n_q], qkv_s[:part, n_q:n_q + n_kv], qkv_s[:part, n_q + n_kv:],
                small_s[2, :head_dim], small_s[2, head_dim:], out_s[:part], small_s[1, :part], gate_s[:part], up_s[:part], down_s)

    return jax.shard_map(device_step, mesh=mesh, in_specs=(row_spec, row_spec, row_spec) + weight_specs + (batch_spec,), out_specs=(batch_spec, row_spec) + weight_specs, check_vma=False)
```
